256 devices in a mesh: rows: 32 (over x, z_lo, core), cols: 8 (over y, z_hi).
Axes of the slice: x: 4, y: 4, z: 8 (z_hi: 2, z_lo: 4; z = z_hi * 4 + z_lo), core: 2. Of those that a mesh axis runs over, the one named last changes fastest.
Arguments:
- image: float32 [2048, 16384], P('rows', 'cols'), may hold values from -6 to 6
- cloud_mask: int32 [2048, 16384], P('rows', 'cols'), may hold values 0 or 1
- tile_weight: int32 [256, 128], P('rows', 'cols'), may hold values from 1 to 8
- owner: int32 [256], replicated, may hold values from 0 to 31, as said below
Outputs:
- solution: float32 [2048, 16384], P('rows', 'cols')
- objective: float32 [3], replicated
The draws below stay inside these ranges and needn't reach their ends.
Inputs may be any that keep to these rules, and one draw needn't show every extreme that they name: `owner`: every index of rows owns exactly 8 blocks, and the 8 blocks b*8 to b*8 + 7 have 8 different owners for every b.
All inputs are finite; a program needn't handle non-finite values. No bound on the sum of `cloud_mask` on one device may be relied on, other than what follows from the above.
Results may differ from the reference program's by a relative error of at most 0.0001.
Values sent between devices are 32-bit elements; how exact they have to be, the bound alone decides.
A program may use at most 64 MiB of HBM per device.

```python
import jax
import jax.numpy as jnp

BR = 8
BPD = 8
W = 16384
TW = 128
ITERS = 3
NBLK = 256
H = 2048
N_ROWS = 32


def draw_owner(key, part):
    folded = jax.random.fold_in(key, 11)
    shuffled = jax.random.permutation(jax.random.fold_in(folded, 1), N_ROWS).astype(jnp.int32)
    ranks = jnp.argsort(shuffled).astype(jnp.int32)
    values = jnp.arange(N_ROWS, dtype=jnp.int32)
    special = ((values == 1) | (values == N_ROWS // 2)).astype(jnp.int32)
    scores = ranks - 2 * N_ROWS * special
    offsets = jnp.argsort(scores).astype(jnp.int32)[:BPD]
    subkeys = jax.random.split(jax.random.fold_in(folded, 2), N_ROWS)
    orders = jax.vmap(lambda sub_key: jax.random.permutation(sub_key, BPD))(subkeys)
    source = jnp.arange(N_ROWS, dtype=jnp.int32)[:, None]
    owners = (source + offsets[orders]) % N_ROWS
    return owners.reshape(-1).astype(jnp.int32)


def set_ends(values, rng, smallest, largest):
    place = [jax.random.randint(jax.random.fold_in(rng, axis), (), 0, length) for axis, length in enumerate(values.shape)]
    longest = values.shape.index(max(values.shape))
    neighbour = place[:longest] + [(place[longest] + 1) % values.shape[longest]] + place[longest + 1:]
    return values.at[tuple(place)].set(smallest).at[tuple(neighbour)].set(largest)


def block_scale(key, extent, pieces, smallest, largest):
    gain = 1.0
    for axis_at, blocks in pieces:
        draws = jax.random.uniform(jax.random.fold_in(jax.random.fold_in(key, 6), axis_at), (blocks,), jnp.float32, smallest / len(pieces), largest / len(pieces))
        gain = gain * jnp.repeat(jnp.exp(draws), extent[axis_at] // blocks).reshape((-1,) + (1,) * (len(extent) - 1 - axis_at))
    return gain


def noise(own_key, dims, deviation, limit, cuts=(), kind=jnp.bfloat16):
    result = deviation * jax.random.normal(own_key, dims, jnp.float32)
    if cuts:
        result = result * block_scale(own_key, dims, cuts, -0.22, 0.18)
    return jnp.clip(result, -limit, limit).astype(kind)


def setup_inputs(seed: int = 0) -> dict:
    key_of = jax.random.split(jax.random.key(seed), 5)
    return {
        "image": noise(key_of[0], (H, W), 1.0, 6.0, ((0, 32), (1, 8)), jnp.float32),
        "cloud_mask": set_ends((jax.random.randint(key_of[1], (H, W), 0, 3) < 1).astype(jnp.int32), jax.random.fold_in(key_of[1], 1), 0, 1),
        "tile_weight": set_ends(jax.random.randint(key_of[2], (NBLK, W // TW), 1, 9), jax.random.fold_in(key_of[2], 1), 1, 8).astype(jnp.int32),
        "owner": draw_owner(jax.random.fold_in(key_of[4], 71), 0),
    }


fidelity_scale = 0.25
tau_step = 0.35
sigma_step = 0.35
tv_weight = 0.3

def forward_rows(field):
    return jnp.concatenate([field[1:] - field[:-1], jnp.zeros_like(field[:1])], axis=0)

def forward_cols(field):
    return jnp.concatenate([field[:, 1:] - field[:, :-1], jnp.zeros_like(field[:, :1])], axis=1)

def divergence(dual_rows, dual_cols):
    above = jnp.concatenate([jnp.zeros_like(dual_rows[:1]), dual_rows[:-1]], axis=0)
    leftward = jnp.concatenate([jnp.zeros_like(dual_cols[:, :1]), dual_cols[:, :-1]], axis=1)
    return dual_rows - above + (dual_cols - leftward)

def reference(image, cloud_mask, tile_weight, owner):
    height, width = image.shape
    total_blocks = owner.shape[0]
    tile_count = tile_weight.shape[1]
    per_tile = jnp.broadcast_to(tile_weight.astype(jnp.float32)[:, None, :, None], (total_blocks, BR, tile_count, TW)).reshape(height, width)
    fidelity = fidelity_scale * per_tile * (1 - cloud_mask).astype(jnp.float32)
    primal = image
    extrap = image
    dual_rows = jnp.zeros_like(image)
    dual_cols = jnp.zeros_like(image)
    objective_list = []
    for step in range(ITERS):
        grad_r = forward_rows(extrap)
        grad_c = forward_cols(extrap)
        trial_rows = dual_rows + sigma_step * grad_r
        trial_cols = dual_cols + sigma_step * grad_c
        shrink = jnp.maximum(1.0, jnp.sqrt(trial_rows * trial_rows + trial_cols * trial_cols) / tv_weight)
        dual_rows = trial_rows / shrink
        dual_cols = trial_cols / shrink
        updated = (primal + tau_step * divergence(dual_rows, dual_cols) + tau_step * fidelity * image) / (1.0 + tau_step * fidelity)
        misfit = updated - image
        total = jnp.sum(0.5 * fidelity * misfit * misfit) + tv_weight * jnp.sum(jnp.sqrt(grad_r * grad_r + grad_c * grad_c))
        objective_list.append(total / (height * width))
        extrap = 2.0 * updated - primal
        primal = updated
    order = jnp.argsort(owner, stable=True)
    solution = primal.reshape(total_blocks, BR, width)[order].reshape(height, width)
    return (solution, jnp.stack(objective_list).astype(jnp.float32))
```

```python
import functools

import jax
import jax.numpy as jnp
from jax import lax
from jax.experimental import pallas as pl
from jax.experimental.pallas import tpu as pltpu
from jax.sharding import PartitionSpec as P

BR = 8
TW = 128
ITERS = 3
HALF = 4

fidelity_scale = 0.25
tau_step = 0.35
sigma_step = 0.35
tv_weight = 0.3

MESH = pl.DeviceIdType.MESH


def kernel(
    n_rows, n_cols, blocks, tiles, pixel_total,
    image_hbm, mask_hbm, weight_ref, owner_ref,
    out_hbm, objective_ref,
    img, fid, gain, bias, prim, ext, dual_r, dual_c, mask_v,
    row_msg, row_got, col_msg, col_got, corner_got,
    staged, spread, sorted_, gathered, out_v,
    order_v, order_s, acc, part_src, part_rows, part_src_c, part_cols,
    load_sem, order_sem, halo_send, halo_recv,
    send1, recv1, send2, recv2, psend, precv, csend, crecv, out_sem,
):
    width = tiles * TW
    ring = width + TW
    r = lax.axis_index("rows")
    c = lax.axis_index("cols")
    up, down = lax.rem(r + n_rows - 1, n_rows), lax.rem(r + 1, n_rows)
    left, right = lax.rem(c + n_cols - 1, n_cols), lax.rem(c + 1, n_cols)

    load_image = pltpu.make_async_copy(image_hbm, img.at[pl.ds(0, blocks), :, pl.ds(0, width)], load_sem.at[0])
    load_mask = pltpu.make_async_copy(mask_hbm, mask_v, load_sem.at[1])
    load_image.start()
    load_mask.start()

    barrier = pltpu.get_barrier_semaphore()

    def greet(row, col):
        pl.semaphore_signal(barrier, inc=1, device_id=(row, col), device_id_type=MESH)

    @pl.loop(1, n_cols)
    def _(j):
        greet(r, lax.rem(c + j, n_cols))

    for row in (up, down):
        for col in (left, right):
            greet(row, col)

    @pl.loop(1, n_rows)
    def _(j):
        greet(lax.rem(r + j, n_rows), c)

    total = n_rows * blocks
    own = jnp.broadcast_to(owner_ref[...], (total, total))
    before = lax.broadcasted_iota(jnp.int32, (total, total), 0)
    after = lax.broadcasted_iota(jnp.int32, (total, total), 1)
    same = (own == own.T) & (before < after)
    rank = jnp.sum(jnp.where(same, 1, 0), axis=0, keepdims=True)
    place = jnp.broadcast_to(owner_ref[...] * blocks + rank, (total, total)).T
    order_v[...] = jnp.sum(jnp.where(place == after, before, 0), axis=0, keepdims=True)
    to_scalars = pltpu.make_async_copy(order_v, order_s, order_sem)
    to_scalars.start()

    load_image.wait()
    load_mask.wait()

    sub = lax.broadcasted_iota(jnp.int32, (BR, ring), 0)
    lane = lax.broadcasted_iota(jnp.int32, (BR, ring), 1)
    sub_w = lax.broadcasted_iota(jnp.int32, (BR, width), 0)

    @pl.loop(0, blocks)
    def _(i):
        weights = jnp.concatenate(
            [jnp.full((BR, TW), weight_ref[i, t].astype(jnp.float32) * fidelity_scale) for t in range(tiles)], axis=1
        )
        fid[i, :, pl.ds(0, width)] = weights * (1 - mask_v[i]).astype(jnp.float32)

    last = blocks - 1
    row_msg[0] = jnp.where(sub_w < HALF, img[0, :, pl.ds(0, width)], pltpu.roll(fid[0, :, pl.ds(0, width)], HALF, 0))
    row_msg[1] = jnp.where(
        sub_w >= HALF, img[last, :, pl.ds(0, width)], pltpu.roll(fid[last, :, pl.ds(0, width)], HALF, 0)
    )
    rows_here = blocks * BR
    for side, start in ((0, 0), (1, width - TW)):
        both = jnp.concatenate(
            [
                img[pl.ds(0, blocks), :, pl.ds(start, TW)].reshape(rows_here, TW),
                fid[pl.ds(0, blocks), :, pl.ds(start, TW)].reshape(rows_here, TW),
            ],
            axis=0,
        ).T
        col_msg[side] = both[:BR] if side == 0 else both[TW - BR :]

    pl.semaphore_wait(barrier, n_rows - 1 + n_cols - 1 + 4)

    first_tile, last_tile = pl.ds(0, TW), pl.ds(width - TW, TW)
    messages = (
        (row_msg.at[0], row_got.at[0], up, c),
        (row_msg.at[1], row_got.at[1], down, c),
        (col_msg.at[0], col_got.at[0], r, left),
        (col_msg.at[1], col_got.at[1], r, right),
        (row_msg.at[0, :, first_tile], corner_got.at[0], up, left),
        (row_msg.at[0, :, last_tile], corner_got.at[1], up, right),
        (row_msg.at[1, :, first_tile], corner_got.at[2], down, left),
        (row_msg.at[1, :, last_tile], corner_got.at[3], down, right),
    )
    halos = [
        pltpu.make_async_remote_copy(
            src_ref=src, dst_ref=dst, send_sem=halo_send.at[k], recv_sem=halo_recv.at[k],
            device_id=(row, col), device_id_type=MESH,
        )
        for k, (src, dst, row, col) in enumerate(messages)
    ]
    for k in (2, 3, 4, 5, 6, 7, 0, 1):
        halos[k].start()
    for halo in halos:
        halo.wait_recv()

    below, above = row_got[0], row_got[1]
    img[blocks, :, pl.ds(0, width)] = jnp.where(sub_w < HALF, below, above)
    fid[blocks, :, pl.ds(0, width)] = pltpu.roll(jnp.where(sub_w < HALF, above, below), HALF, 0)
    sides = jnp.concatenate([col_got[0], jnp.zeros((TW - 2 * BR, TW), jnp.float32), col_got[1]], axis=0).T
    img[pl.ds(0, blocks), :, pl.ds(width, TW)] = sides[:rows_here].reshape(blocks, BR, TW)
    fid[pl.ds(0, blocks), :, pl.ds(width, TW)] = sides[rows_here:].reshape(blocks, BR, TW)
    sub_t = lax.broadcasted_iota(jnp.int32, (BR, TW), 0)
    lane_t = lax.broadcasted_iota(jnp.int32, (BR, TW), 1)
    low = jnp.where(lane_t < TW // 2, corner_got[0], corner_got[1])
    high = jnp.where(lane_t < TW // 2, corner_got[2], corner_got[3])
    img[blocks, :, pl.ds(width, TW)] = jnp.where(sub_t < HALF, low, high)
    fid[blocks, :, pl.ds(width, TW)] = pltpu.roll(jnp.where(sub_t < HALF, high, low), HALF, 0)

    @pl.loop(0, blocks + 1)
    def _(i):
        f = fid[i] * tau_step
        g = 1.0 / (1.0 + f)
        v = img[i]
        gain[i] = g
        bias[i] = f * v * g
        prim[i] = v
        ext[i] = v
        zero = jnp.zeros_like(v)
        dual_r[i] = zero
        dual_c[i] = zero

    edge_col = jnp.where(c == n_cols - 1, width - 1, jnp.where(c == 0, ring - 1, -1))

    def folded(x):
        parts = [x[:, t * TW : (t + 1) * TW] for t in range(tiles)]
        while len(parts) > 1:
            parts = [a + b for a, b in zip(parts[::2], parts[1::2])]
        return parts[0]

    def dual_step(i, following, edge_row):
        e = ext[i]
        lower = jnp.where(sub == BR - 1, pltpu.roll(ext[following], BR - 1, 0), pltpu.roll(e, BR - 1, 0))
        grad_r = jnp.where(sub == edge_row, 0.0, lower - e)
        grad_c = jnp.where(lane == edge_col, 0.0, pltpu.roll(e, ring - 1, 1) - e)
        trial_r = dual_r[i] + sigma_step * grad_r
        trial_c = dual_c[i] + sigma_step * grad_c
        scale = jnp.minimum(1.0, tv_weight * lax.rsqrt(trial_r * trial_r + trial_c * trial_c))
        dual_r[i] = trial_r * scale
        dual_c[i] = trial_c * scale
        return grad_r, grad_c

    def primal_step(i, previous):
        dr, dc, p = dual_r[i], dual_c[i], prim[i]
        upper = jnp.where(sub == 0, pltpu.roll(dual_r[previous], 1, 0), pltpu.roll(dr, 1, 0))
        div = dr - upper + (dc - pltpu.roll(dc, 1, 1))
        updated = (p + tau_step * div) * gain[i] + bias[i]
        ext[i] = 2.0 * updated - p
        prim[i] = updated
        return updated

    @pl.loop(0, ITERS)
    def _(step):
        dual_step(blocks, 0, jnp.where(r == 0, BR - 1, BR))

        def body(i, partial):
            edge_row = jnp.where((i == last) & (r == n_rows - 1), BR - 1, BR)
            grad_r, grad_c = dual_step(i, i + 1, edge_row)
            partial += tv_weight * folded(jnp.sqrt(grad_r * grad_r + grad_c * grad_c))
            misfit = primal_step(i, jnp.where(i == 0, blocks, i - 1)) - img[i]
            return partial + 0.5 * folded(fid[i] * misfit * misfit)

        acc[step] = lax.fori_loop(0, blocks, body, jnp.zeros((BR, TW), jnp.float32))
        primal_step(blocks, last)

    lane_1 = lax.broadcasted_iota(jnp.int32, (1, TW), 1)
    sums = jnp.zeros((1, TW), jnp.float32)
    for step in range(ITERS):
        line = jnp.sum(acc[step], axis=0, keepdims=True)
        sums = jnp.where(lane_1 == step, jnp.sum(line, axis=1, keepdims=True), sums)
    part_src[...] = sums
    part_rows[r] = sums

    @pl.loop(0, blocks)
    def _(i):
        p = prim[i]
        for t in range(tiles):
            tile = p[:, t * TW : (t + 1) * TW]
            staged[2 * t, i] = tile[:HALF]
            staged[2 * t + 1, i] = tile[HALF:]

    def spread_to(m):
        return pltpu.make_async_remote_copy(
            src_ref=staged.at[m], dst_ref=spread.at[r], send_sem=send1, recv_sem=recv1,
            device_id=(m, c), device_id_type=MESH,
        )

    def part_to(m):
        return pltpu.make_async_remote_copy(
            src_ref=part_src, dst_ref=part_rows.at[r], send_sem=psend, recv_sem=precv,
            device_id=(m, c), device_id_type=MESH,
        )

    @pl.loop(1, n_rows)
    def _(j):
        spread_to(lax.rem(r + j, n_rows)).start()

    @pl.loop(1, n_rows)
    def _(j):
        part_to(lax.rem(r + j, n_rows)).start()

    spread[r] = staged[r]
    to_scalars.wait()
    peers = pl.ds(0, n_rows - 1)
    all_spread = pltpu.make_async_remote_copy(
        src_ref=staged.at[peers], dst_ref=spread.at[peers], send_sem=send1, recv_sem=recv1,
        device_id=(up, c), device_id_type=MESH,
    )
    all_spread.wait_recv()

    def collect_to(d):
        return pltpu.make_async_remote_copy(
            src_ref=sorted_.at[d], dst_ref=gathered.at[r], send_sem=send2, recv_sem=recv2,
            device_id=(d, c), device_id_type=MESH,
        )

    def sort_for(d):
        for k in range(blocks):
            b = order_s[0, d * blocks + k]
            sorted_[d, k] = spread[b // blocks, lax.rem(b, blocks)]

    sort_for(lax.rem(r + 1, n_rows))

    @pl.loop(2, n_rows)
    def _(j):
        sort_for(lax.rem(r + j, n_rows))
        collect_to(lax.rem(r + j - 1, n_rows)).start()

    sort_for(r)
    collect_to(up).start()
    gathered[r] = sorted_[r]

    all_parts = pltpu.make_async_remote_copy(
        src_ref=part_rows.at[peers], dst_ref=part_rows.at[peers], send_sem=psend, recv_sem=precv,
        device_id=(up, c), device_id_type=MESH,
    )
    all_parts.wait_recv()
    here = part_rows[0]
    for s in range(1, n_rows):
        here = here + part_rows[s]
    part_src_c[...] = here
    part_cols[c] = here

    def part_across(col):
        return pltpu.make_async_remote_copy(
            src_ref=part_src_c, dst_ref=part_cols.at[c], send_sem=csend, recv_sem=crecv,
            device_id=(r, col), device_id_type=MESH,
        )

    @pl.loop(1, n_cols)
    def _(j):
        part_across(lax.rem(c + j, n_cols)).start()

    col_peers = pl.ds(0, n_cols - 1)
    all_cols = pltpu.make_async_remote_copy(
        src_ref=part_cols.at[col_peers], dst_ref=part_cols.at[col_peers], send_sem=csend, recv_sem=crecv,
        device_id=(r, left), device_id_type=MESH,
    )
    all_cols.wait_recv()
    everywhere = part_cols[0]
    for s in range(1, n_cols):
        everywhere = everywhere + part_cols[s]
    for step in range(ITERS):
        objective_ref[step] = jnp.sum(jnp.where(lane_1 == step, everywhere, 0.0)) / pixel_total

    all_collected = pltpu.make_async_remote_copy(
        src_ref=sorted_.at[peers], dst_ref=gathered.at[peers], send_sem=send2, recv_sem=recv2,
        device_id=(up, c), device_id_type=MESH,
    )
    all_collected.wait_recv()

    @pl.loop(0, blocks)
    def _(k):
        for t in range(tiles):
            out_v[k, :, pl.ds(t * TW, TW)] = jnp.concatenate([gathered[2 * t, k], gathered[2 * t + 1, k]], axis=0)

    store = pltpu.make_async_copy(out_v, out_hbm, out_sem)
    store.start()
    for halo in halos:
        halo.wait_send()
    all_spread.wait_send()
    all_parts.wait_send()
    all_cols.wait_send()
    all_collected.wait_send()
    store.wait()


def per_device(n_rows, n_cols, image, cloud_mask, tile_weight, owner):
    rows_here, width = image.shape
    blocks = rows_here // BR
    tiles = width // TW
    pixel_total = float(n_rows * n_cols * rows_here * width)
    f32 = jnp.float32
    ringed = pltpu.VMEM((blocks + 1, BR, width + TW), f32)
    pieces = pltpu.VMEM((n_rows, blocks, HALF, TW), f32)
    dma = pltpu.SemaphoreType.DMA
    scratch = (
        [ringed] * 8
        + [
            pltpu.VMEM((blocks, BR, width), jnp.int32),
            pltpu.VMEM((2, BR, width), f32),
            pltpu.VMEM((2, BR, width), f32),
            pltpu.VMEM((2, BR, TW), f32),
            pltpu.VMEM((2, BR, TW), f32),
            pltpu.VMEM((4, BR, TW), f32),
        ]
        + [pieces] * 4
        + [
            pltpu.VMEM((blocks, BR, width), f32),
            pltpu.VMEM((1, n_rows * blocks), jnp.int32),
            pltpu.SMEM((1, n_rows * blocks), jnp.int32),
            pltpu.VMEM((ITERS, BR, TW), f32),
            pltpu.VMEM((1, TW), f32),
            pltpu.VMEM((n_rows, 1, TW), f32),
            pltpu.VMEM((1, TW), f32),
            pltpu.VMEM((n_cols, 1, TW), f32),
            dma((2,)), dma, dma((8,)), dma((8,)),
            dma, dma, dma, dma, dma, dma, dma, dma, dma,
        ]
    )
    vmem, smem, hbm = (pl.BlockSpec(memory_space=s) for s in (pltpu.VMEM, pltpu.SMEM, pl.ANY))
    out, objective = pl.pallas_call(
        functools.partial(kernel, n_rows, n_cols, blocks, tiles, pixel_total),
        out_shape=(
            jax.ShapeDtypeStruct((blocks, BR, width), f32),
            jax.ShapeDtypeStruct((ITERS,), f32),
        ),
        in_specs=[hbm, hbm, smem, vmem],
        out_specs=(hbm, smem),
        scratch_shapes=scratch,
        compiler_params=pltpu.CompilerParams(collective_id=0, has_side_effects=True),
    )(
        image.reshape(blocks, BR, width),
        cloud_mask.reshape(blocks, BR, width),
        tile_weight,
        owner.reshape(1, -1),
    )
    return out.reshape(rows_here, width), objective


def solution(mesh):
    placed = (P("rows", "cols"), P("rows", "cols"), P("rows", "cols"), P())
    return jax.shard_map(
        functools.partial(per_device, mesh.shape["rows"], mesh.shape["cols"]),
        mesh=mesh, in_specs=placed, out_specs=(P("rows", "cols"), P()), check_vma=False,
    )
```

```python
import functools

import jax
import jax.numpy as jnp
from jax import lax
from jax.experimental import pallas as pl
from jax.experimental.pallas import tpu as pltpu
from jax.sharding import PartitionSpec as P

BR = 8
TW = 128
ITERS = 3
HALF = 4

fidelity_scale = 0.25
tau_step = 0.35
sigma_step = 0.35
tv_weight = 0.3

MESH = pl.DeviceIdType.MESH


def kernel(
    n_rows, n_cols, blocks, tiles, pixel_total,
    image_hbm, mask_hbm, weight_ref, owner_ref,
    out_hbm, objective_ref,
    img, fid, gain, bias, prim, ext, dual_r, dual_c,
    strip_prim, strip_ext, strip_r, strip_c, side_prim, side_ext, side_r, side_c, mask_v,
    row_msg, row_got, col_msg, col_got, corner_got,
    staged, spread, sorted_, gathered, out_v,
    order_v, order_s, acc, part_src, part_rows, part_src_c, part_cols,
    load_sem, order_sem, halo_send, halo_recv,
    send1, recv1, send2, recv2, psend, precv, csend, crecv, out_sem,
):
    width = tiles * TW
    ring = width + TW
    r = lax.axis_index("rows")
    c = lax.axis_index("cols")
    up, down = lax.rem(r + n_rows - 1, n_rows), lax.rem(r + 1, n_rows)
    left, right = lax.rem(c + n_cols - 1, n_cols), lax.rem(c + 1, n_cols)

    load_image = pltpu.make_async_copy(image_hbm, img.at[pl.ds(0, blocks), :, pl.ds(0, width)], load_sem.at[0])
    load_mask = pltpu.make_async_copy(mask_hbm, mask_v, load_sem.at[1])
    load_image.start()
    load_mask.start()

    barrier = pltpu.get_barrier_semaphore()

    def greet(row, col):
        pl.semaphore_signal(barrier, inc=1, device_id=(row, col), device_id_type=MESH)

    @pl.loop(1, n_cols)
    def _(j):
        greet(r, lax.rem(c + j, n_cols))

    for row in (up, down):
        for col in (left, right):
            greet(row, col)

    @pl.loop(1, n_rows)
    def _(j):
        greet(lax.rem(r + j, n_rows), c)

    total = n_rows * blocks
    own = jnp.broadcast_to(owner_ref[...], (total, total))
    before = lax.broadcasted_iota(jnp.int32, (total, total), 0)
    after = lax.broadcasted_iota(jnp.int32, (total, total), 1)
    same = (own == own.T) & (before < after)
    rank = jnp.sum(jnp.where(same, 1, 0), axis=0, keepdims=True)
    place = jnp.broadcast_to(owner_ref[...] * blocks + rank, (total, total)).T
    order_v[...] = jnp.sum(jnp.where(place == after, before, 0), axis=0, keepdims=True)
    to_scalars = pltpu.make_async_copy(order_v, order_s, order_sem)
    to_scalars.start()

    load_image.wait()
    load_mask.wait()

    sub = lax.broadcasted_iota(jnp.int32, (BR, TW), 0)
    lane = lax.broadcasted_iota(jnp.int32, (BR, TW), 1)
    sub_w = lax.broadcasted_iota(jnp.int32, (BR, width), 0)
    last, last_t = blocks - 1, tiles - 1

    def at(t):
        return pl.ds(t * TW if isinstance(t, int) else pl.multiple_of(t * TW, TW), TW)

    def coefficients(i, where):
        f = fid[i, :, where] * tau_step
        g = 1.0 / (1.0 + f)
        gain[i, :, where] = g
        bias[i, :, where] = f * img[i, :, where] * g

    @pl.loop(0, blocks)
    def _(i):
        for t in range(tiles):
            weight = weight_ref[i, t].astype(jnp.float32) * fidelity_scale
            fid[i, :, at(t)] = weight * (1 - mask_v[i, :, at(t)]).astype(jnp.float32)
            coefficients(i, at(t))

    row_msg[0] = jnp.where(sub_w < HALF, img[0, :, pl.ds(0, width)], pltpu.roll(fid[0, :, pl.ds(0, width)], HALF, 0))
    row_msg[1] = jnp.where(
        sub_w >= HALF, img[last, :, pl.ds(0, width)], pltpu.roll(fid[last, :, pl.ds(0, width)], HALF, 0)
    )
    rows_here = blocks * BR
    for side, start in ((0, 0), (1, width - TW)):
        both = jnp.concatenate(
            [
                img[pl.ds(0, blocks), :, pl.ds(start, TW)].reshape(rows_here, TW),
                fid[pl.ds(0, blocks), :, pl.ds(start, TW)].reshape(rows_here, TW),
            ],
            axis=0,
        ).T
        col_msg[side] = both[:BR] if side == 0 else both[TW - BR :]

    def dual_update(e, e_right, e_below, dr, dc, no_row=None, no_col=None):
        grad_r = pltpu.roll(jnp.where(sub == 0, e_below, e), BR - 1, 0) - e
        grad_c = pltpu.roll(jnp.where(lane == 0, e_right, e), TW - 1, 1) - e
        if no_row is not None:
            grad_r = jnp.where(sub == no_row, 0.0, grad_r)
        if no_col is not None:
            grad_c = jnp.where(lane == no_col, 0.0, grad_c)
        trial_r = sigma_step * grad_r
        trial_c = sigma_step * grad_c
        if dr is not None:
            trial_r, trial_c = dr + trial_r, dc + trial_c
        scale = jnp.minimum(1.0, tv_weight * lax.rsqrt(trial_r * trial_r + trial_c * trial_c))
        return trial_r * scale, trial_c * scale, jnp.sqrt(grad_r * grad_r + grad_c * grad_c)

    def primal_update(p, dr, dc, dr_above, dc_left, g, b):
        upper = pltpu.roll(jnp.where(sub == BR - 1, dr_above, dr), 1, 0)
        before = pltpu.roll(jnp.where(lane == TW - 1, dc_left, dc), 1, 1)
        return (p + tau_step * ((dr - upper) + (dc - before))) * g + b

    def loss(variation, f, misfit):
        return tv_weight * variation + 0.5 * f * (misfit * misfit)

    for step in range(ITERS):
        old = img if step == 0 else ext
        old_prim = img if step == 0 else prim

        def body(i, partial, step=step, old=old, old_prim=old_prim):
            following, previous = jnp.minimum(i + 1, last), jnp.maximum(i - 1, 0)
            row = jnp.zeros((BR, TW), jnp.float32)
            e = old[i, :, at(0)]
            dc_left = None
            for t in range(tiles):
                e_right = old[i, :, at(min(t + 1, last_t))]
                dr, dc = (None, None) if step == 0 else (dual_r[i, :, at(t)], dual_c[i, :, at(t)])
                dr, dc, variation = dual_update(e, e_right, old[following, :, at(t)], dr, dc)
                dual_r[i, :, at(t)] = dr
                dual_c[i, :, at(t)] = dc
                p = old_prim[i, :, at(t)]
                updated = primal_update(
                    p, dr, dc, dual_r[previous, :, at(t)], dc if t == 0 else dc_left, gain[i, :, at(t)], bias[i, :, at(t)]
                )
                dc_left = dc
                if step < ITERS - 1:
                    ext[i, :, at(t)] = 2.0 * updated - p
                else:
                    staged[2 * t, i] = updated[:HALF]
                    staged[2 * t + 1, i] = updated[HALF:]
                prim[i, :, at(t)] = updated
                term = loss(variation, fid[i, :, at(t)], updated - img[i, :, at(t)])
                if t == 0:
                    term = jnp.where(lane >= TW // 2, term, 0.0)
                if t == last_t:
                    term = jnp.where(lane < TW // 2, term, 0.0)
                row = row + term
                e = e_right
            first = jnp.where(i == 0, HALF, 0)
            end = jnp.where(i == last, HALF, BR)
            return partial + jnp.where((sub >= first) & (sub < end), row, 0.0)

        acc[step] = lax.fori_loop(0, blocks, body, jnp.zeros((BR, TW), jnp.float32))

    pl.semaphore_wait(barrier, n_rows - 1 + n_cols - 1 + 4)

    first_tile, last_tile = pl.ds(0, TW), pl.ds(width - TW, TW)
    messages = (
        (row_msg.at[0], row_got.at[0], up, c),
        (row_msg.at[1], row_got.at[1], down, c),
        (col_msg.at[0], col_got.at[0], r, left),
        (col_msg.at[1], col_got.at[1], r, right),
        (row_msg.at[0, :, first_tile], corner_got.at[0], up, left),
        (row_msg.at[0, :, last_tile], corner_got.at[1], up, right),
        (row_msg.at[1, :, first_tile], corner_got.at[2], down, left),
        (row_msg.at[1, :, last_tile], corner_got.at[3], down, right),
    )
    halos = [
        pltpu.make_async_remote_copy(
            src_ref=src, dst_ref=dst, send_sem=halo_send.at[k], recv_sem=halo_recv.at[k],
            device_id=(row, col), device_id_type=MESH,
        )
        for k, (src, dst, row, col) in enumerate(messages)
    ]
    for k in (2, 3, 4, 5, 6, 7, 0, 1):
        halos[k].start()

    def spread_to(m, start, size):
        piece = pl.ds(start, size)
        return pltpu.make_async_remote_copy(
            src_ref=staged.at[m, piece], dst_ref=spread.at[r, piece], send_sem=send1, recv_sem=recv1,
            device_id=(m, c), device_id_type=MESH,
        )

    @pl.loop(1, n_rows)
    def _(j):
        m = lax.rem(r + j, n_rows)

        @pl.when((m >= 2) & (m < n_rows - 2))
        def _():
            spread_to(m, 1 - lax.rem(m, 2), last).start()

    for halo in halos:
        halo.wait_recv()

    below, above = row_got[0], row_got[1]
    img[blocks, :, pl.ds(0, width)] = jnp.where(sub_w < HALF, below, above)
    fid[blocks, :, pl.ds(0, width)] = pltpu.roll(jnp.where(sub_w < HALF, above, below), HALF, 0)
    sides = jnp.concatenate([col_got[0], jnp.zeros((TW - 2 * BR, TW), jnp.float32), col_got[1]], axis=0).T
    img[pl.ds(0, blocks), :, pl.ds(width, TW)] = sides[:rows_here].reshape(blocks, BR, TW)
    fid[pl.ds(0, blocks), :, pl.ds(width, TW)] = sides[rows_here:].reshape(blocks, BR, TW)
    low = jnp.where(lane < TW // 2, corner_got[0], corner_got[1])
    high = jnp.where(lane < TW // 2, corner_got[2], corner_got[3])
    img[blocks, :, pl.ds(width, TW)] = jnp.where(sub < HALF, low, high)
    fid[blocks, :, pl.ds(width, TW)] = pltpu.roll(jnp.where(sub < HALF, high, low), HALF, 0)

    coefficients(blocks, pl.ds(0, ring))
    for i in range(blocks):
        coefficients(i, at(tiles))

    zero = jnp.zeros((BR, TW), jnp.float32)

    rows_of = (last, blocks, 0)
    no_rows = (jnp.where(r == n_rows - 1, BR - 1, BR), jnp.where(r == 0, BR - 1, BR), None)
    group = 4

    for step in range(ITERS):

        def strip_body(q, partial, step=step):
            def source(refs, k, t):
                return img[rows_of[k], :, at(t)] if step == 0 else refs[k, :, at(t)]

            for n in range(group):
                t = q * group + n
                before, after = jnp.maximum(t - 1, 0), jnp.minimum(t + 1, last_t)
                e = [source(strip_ext, k, t) for k in range(3)]
                duals = []
                for k in range(3):
                    dr, dc = (None, None) if step == 0 else (strip_r[k, :, at(t)], strip_c[k, :, at(t)])
                    duals.append(
                        dual_update(e[k], source(strip_ext, k, after), e[(k + 1) % 3], dr, dc, no_row=no_rows[k])
                    )
                for k in range(3):
                    dr, dc, variation = duals[k]
                    dc_left = strip_c[k, :, at(before)] if n or step else jnp.where(q == 0, dc, strip_c[k, :, at(before)])
                    strip_r[k, :, at(t)] = dr
                    strip_c[k, :, at(t)] = dc
                    p = source(strip_prim, k, t)
                    i = rows_of[k]
                    updated = primal_update(
                        p, dr, dc, duals[(k + 2) % 3][0], dc_left, gain[i, :, at(t)], bias[i, :, at(t)]
                    )
                    if step < ITERS - 1:
                        strip_ext[k, :, at(t)] = 2.0 * updated - p
                    strip_prim[k, :, at(t)] = updated
                    if k != 1:
                        term = loss(variation, fid[i, :, at(t)], updated - img[i, :, at(t)])
                        keep = sub < HALF if k == 2 else sub >= HALF
                        if n == 0:
                            keep = keep & (lane >= jnp.where(q == 0, TW // 2, 0))
                        if n == group - 1:
                            keep = keep & (lane < jnp.where(t == last_t, TW // 2, TW))
                        partial = partial + jnp.where(keep, term, 0.0)
            return partial

        acc[step] = lax.fori_loop(0, tiles // group, strip_body, acc[step])

    cols_of = (last_t, tiles, 0)
    no_cols = (jnp.where(c == n_cols - 1, TW - 1, TW), jnp.where(c == 0, TW - 1, TW), None)
    for step in range(ITERS):
        partial = acc[step]
        e = [
            [img[i, :, at(cols_of[k])] if step == 0 else side_ext[i, :, at(k)] for k in range(3)]
            for i in range(blocks + 1)
        ]
        variations = {}
        for i in range(blocks + 1):
            no_row = no_rows[0] if i == last else no_rows[1] if i == blocks else None
            for k in range(3):
                dr, dc = (None, None) if step == 0 else (side_r[i, :, at(k)], side_c[i, :, at(k)])
                dr, dc, variations[i, k] = dual_update(
                    e[i][k], e[i][(k + 1) % 3], e[(i + 1) % (blocks + 1)][k], dr, dc, no_row=no_row, no_col=no_cols[k]
                )
                side_r[i, :, at(k)] = dr
                side_c[i, :, at(k)] = dc
        for i in range(blocks + 1):
            for k in range(3):
                t = cols_of[k]
                p = img[i, :, at(t)] if step == 0 else side_prim[i, :, at(k)]
                updated = primal_update(
                    p, side_r[i, :, at(k)], side_c[i, :, at(k)], side_r[(i + blocks) % (blocks + 1), :, at(k)],
                    side_c[i, :, at((k + 2) % 3)], gain[i, :, at(t)], bias[i, :, at(t)],
                )
                if step < ITERS - 1:
                    side_ext[i, :, at(k)] = 2.0 * updated - p
                side_prim[i, :, at(k)] = updated
                if k != 1 and i < blocks:
                    term = loss(variations[i, k], fid[i, :, at(t)], updated - img[i, :, at(t)])
                    partial = partial + jnp.where(lane < TW // 2 if k == 2 else lane >= TW // 2, term, 0.0)
        acc[step] = partial

    for t in range(1, last_t):
        staged[2 * t, 0] = strip_prim[2, :HALF, at(t)]
        staged[2 * t + 1, last] = strip_prim[0, HALF:, at(t)]
    for k, t in ((2, 0), (0, last_t)):
        for i in range(blocks):
            value = prim[i, :, at(t)]
            if i == 0:
                value = jnp.where(sub < HALF, strip_prim[2, :, at(t)], value)
            if i == last:
                value = jnp.where(sub >= HALF, strip_prim[0, :, at(t)], value)
            value = jnp.where(lane < TW // 2 if k == 2 else lane >= TW // 2, side_prim[i, :, at(k)], value)
            staged[2 * t, i] = value[:HALF]
            staged[2 * t + 1, i] = value[HALF:]

    lane_1 = lax.broadcasted_iota(jnp.int32, (1, TW), 1)
    sums = jnp.zeros((1, TW), jnp.float32)
    for step in range(ITERS):
        line = jnp.sum(acc[step], axis=0, keepdims=True)
        sums = jnp.where(lane_1 == step, jnp.sum(line, axis=1, keepdims=True), sums)
    part_src[...] = sums
    part_rows[r] = sums

    def part_to(m):
        return pltpu.make_async_remote_copy(
            src_ref=part_src, dst_ref=part_rows.at[r], send_sem=psend, recv_sem=precv,
            device_id=(m, c), device_id_type=MESH,
        )

    @pl.loop(1, n_rows)
    def _(j):
        m = lax.rem(r + j, n_rows)
        inner = (m >= 2) & (m < n_rows - 2)

        @pl.when(inner)
        def _():
            spread_to(m, last * lax.rem(m, 2), 1).start()

        @pl.when(jnp.logical_not(inner))
        def _():
            spread_to(m, 0, blocks).start()

    @pl.loop(1, n_rows)
    def _(j):
        part_to(lax.rem(r + j, n_rows)).start()

    spread[r] = staged[r]
    to_scalars.wait()
    peers = pl.ds(0, n_rows - 1)
    all_spread = pltpu.make_async_remote_copy(
        src_ref=staged.at[peers], dst_ref=spread.at[peers], send_sem=send1, recv_sem=recv1,
        device_id=(up, c), device_id_type=MESH,
    )
    all_spread.wait_recv()

    def collect_to(d):
        return pltpu.make_async_remote_copy(
            src_ref=sorted_.at[d], dst_ref=gathered.at[r], send_sem=send2, recv_sem=recv2,
            device_id=(d, c), device_id_type=MESH,
        )

    def sort_for(d):
        for k in range(blocks):
            b = order_s[0, d * blocks + k]
            sorted_[d, k] = spread[b // blocks, lax.rem(b, blocks)]

    sort_for(lax.rem(r + 1, n_rows))

    @pl.loop(2, n_rows)
    def _(j):
        sort_for(lax.rem(r + j, n_rows))
        collect_to(lax.rem(r + j - 1, n_rows)).start()

    sort_for(r)
    collect_to(up).start()
    gathered[r] = sorted_[r]

    all_parts = pltpu.make_async_remote_copy(
        src_ref=part_rows.at[peers], dst_ref=part_rows.at[peers], send_sem=psend, recv_sem=precv,
        device_id=(up, c), device_id_type=MESH,
    )
    all_parts.wait_recv()
    here = part_rows[0]
    for s in range(1, n_rows):
        here = here + part_rows[s]
    part_src_c[...] = here
    part_cols[c] = here

    def part_across(col):
        return pltpu.make_async_remote_copy(
            src_ref=part_src_c, dst_ref=part_cols.at[c], send_sem=csend, recv_sem=crecv,
            device_id=(r, col), device_id_type=MESH,
        )

    @pl.loop(1, n_cols)
    def _(j):
        part_across(lax.rem(c + j, n_cols)).start()

    col_peers = pl.ds(0, n_cols - 1)
    all_cols = pltpu.make_async_remote_copy(
        src_ref=part_cols.at[col_peers], dst_ref=part_cols.at[col_peers], send_sem=csend, recv_sem=crecv,
        device_id=(r, left), device_id_type=MESH,
    )
    all_cols.wait_recv()
    everywhere = part_cols[0]
    for s in range(1, n_cols):
        everywhere = everywhere + part_cols[s]
    for step in range(ITERS):
        objective_ref[step] = jnp.sum(jnp.where(lane_1 == step, everywhere, 0.0)) / pixel_total

    all_collected = pltpu.make_async_remote_copy(
        src_ref=sorted_.at[peers], dst_ref=gathered.at[peers], send_sem=send2, recv_sem=recv2,
        device_id=(up, c), device_id_type=MESH,
    )
    all_collected.wait_recv()

    @pl.loop(0, blocks)
    def _(k):
        for t in range(tiles):
            out_v[k, :, pl.ds(t * TW, TW)] = jnp.concatenate([gathered[2 * t, k], gathered[2 * t + 1, k]], axis=0)

    store = pltpu.make_async_copy(out_v, out_hbm, out_sem)
    store.start()
    for halo in halos:
        halo.wait_send()
    all_spread.wait_send()
    all_parts.wait_send()
    all_cols.wait_send()
    all_collected.wait_send()
    store.wait()


def per_device(n_rows, n_cols, image, cloud_mask, tile_weight, owner):
    rows_here, width = image.shape
    blocks = rows_here // BR
    tiles = width // TW
    pixel_total = float(n_rows * n_cols * rows_here * width)
    f32 = jnp.float32
    ringed = pltpu.VMEM((blocks + 1, BR, width + TW), f32)
    pieces = pltpu.VMEM((n_rows, blocks, HALF, TW), f32)
    dma = pltpu.SemaphoreType.DMA
    scratch = (
        [ringed] * 4
        + [pltpu.VMEM((blocks, BR, width), f32)] * 4
        + [pltpu.VMEM((3, BR, width), f32)] * 4
        + [pltpu.VMEM((blocks + 1, BR, 3 * TW), f32)] * 4
        + [
            pltpu.VMEM((blocks, BR, width), jnp.int32),
            pltpu.VMEM((2, BR, width), f32),
            pltpu.VMEM((2, BR, width), f32),
            pltpu.VMEM((2, BR, TW), f32),
            pltpu.VMEM((2, BR, TW), f32),
            pltpu.VMEM((4, BR, TW), f32),
        ]
        + [pieces] * 4
        + [
            pltpu.VMEM((blocks, BR, width), f32),
            pltpu.VMEM((1, n_rows * blocks), jnp.int32),
            pltpu.SMEM((1, n_rows * blocks), jnp.int32),
            pltpu.VMEM((ITERS, BR, TW), f32),
            pltpu.VMEM((1, TW), f32),
            pltpu.VMEM((n_rows, 1, TW), f32),
            pltpu.VMEM((1, TW), f32),
            pltpu.VMEM((n_cols, 1, TW), f32),
            dma((2,)), dma, dma((8,)), dma((8,)),
            dma, dma, dma, dma, dma, dma, dma, dma, dma,
        ]
    )
    vmem, smem, hbm = (pl.BlockSpec(memory_space=s) for s in (pltpu.VMEM, pltpu.SMEM, pl.ANY))
    out, objective = pl.pallas_call(
        functools.partial(kernel, n_rows, n_cols, blocks, tiles, pixel_total),
        out_shape=(
            jax.ShapeDtypeStruct((blocks, BR, width), f32),
            jax.ShapeDtypeStruct((ITERS,), f32),
        ),
        in_specs=[hbm, hbm, smem, vmem],
        out_specs=(hbm, smem),
        scratch_shapes=scratch,
        compiler_params=pltpu.CompilerParams(collective_id=0, has_side_effects=True),
    )(
        image.reshape(blocks, BR, width),
        cloud_mask.reshape(blocks, BR, width),
        tile_weight,
        owner.reshape(1, -1),
    )
    return out.reshape(rows_here, width), objective


def solution(mesh):
    placed = (P("rows", "cols"), P("rows", "cols"), P("rows", "cols"), P())
    return jax.shard_map(
        functools.partial(per_device, mesh.shape["rows"], mesh.shape["cols"]),
        mesh=mesh, in_specs=placed, out_specs=(P("rows", "cols"), P()), check_vma=False,
    )
```

```python
import functools

import jax
import jax.numpy as jnp
from jax import lax
from jax.experimental import pallas as pl
from jax.experimental.pallas import tpu as pltpu
from jax.sharding import PartitionSpec as P

BR = 8
TW = 128
ITERS = 3
HALF = 4

fidelity_scale = 0.25
tau_step = 0.35
sigma_step = 0.35
tv_weight = 0.3

MESH = pl.DeviceIdType.MESH


def kernel(
    n_rows, n_cols, blocks, tiles, pixel_total,
    image_hbm, mask_hbm, weight_ref, owner_ref,
    out_hbm, objective_ref,
    img, fid, gain, bias, prim, ext, dual_r, dual_c,
    strip_prim, strip_ext, strip_r, strip_c, side_prim, side_ext, side_r, side_c, mask_v,
    row_msg, row_got, col_msg, col_got, corner_got,
    staged, spread, sorted_, gathered, out_v,
    order_v, order_s, acc, part_src, part_rows, part_src_c, part_cols,
    load_sem, order_sem, halo_send, halo_recv,
    send1, recv1, send2, recv2, psend, precv, csend, crecv, out_sem,
):
    width = tiles * TW
    ring = width + TW
    r = lax.axis_index("rows")
    c = lax.axis_index("cols")
    up, down = lax.rem(r + n_rows - 1, n_rows), lax.rem(r + 1, n_rows)
    left, right = lax.rem(c + n_cols - 1, n_cols), lax.rem(c + 1, n_cols)

    load_image = pltpu.make_async_copy(image_hbm, img.at[pl.ds(0, blocks), :, pl.ds(0, width)], load_sem.at[0])
    load_mask = pltpu.make_async_copy(mask_hbm, mask_v, load_sem.at[1])
    load_image.start()
    load_mask.start()

    barrier = pltpu.get_barrier_semaphore()

    def greet(row, col):
        pl.semaphore_signal(barrier, inc=1, device_id=(row, col), device_id_type=MESH)

    @pl.loop(1, n_cols)
    def _(j):
        greet(r, lax.rem(c + j, n_cols))

    for row in (up, down):
        for col in (left, right):
            greet(row, col)

    @pl.loop(1, n_rows)
    def _(j):
        greet(lax.rem(r + j, n_rows), c)

    total = n_rows * blocks
    own = jnp.broadcast_to(owner_ref[...], (total, total))
    before = lax.broadcasted_iota(jnp.int32, (total, total), 0)
    after = lax.broadcasted_iota(jnp.int32, (total, total), 1)
    same = (own == own.T) & (before < after)
    rank = jnp.sum(jnp.where(same, 1, 0), axis=0, keepdims=True)
    place = jnp.broadcast_to(owner_ref[...] * blocks + rank, (total, total)).T
    order_v[...] = jnp.sum(jnp.where(place == after, before, 0), axis=0, keepdims=True)
    to_scalars = pltpu.make_async_copy(order_v, order_s, order_sem)
    to_scalars.start()

    load_image.wait()
    load_mask.wait()

    sub = lax.broadcasted_iota(jnp.int32, (BR, TW), 0)
    lane = lax.broadcasted_iota(jnp.int32, (BR, TW), 1)
    sub_w = lax.broadcasted_iota(jnp.int32, (BR, width), 0)
    last, last_t = blocks - 1, tiles - 1

    def at(t):
        return pl.ds(t * TW if isinstance(t, int) else pl.multiple_of(t * TW, TW), TW)

    def coefficients(i, where):
        f = fid[i, :, where] * tau_step
        g = 1.0 / (1.0 + f)
        gain[i, :, where] = g
        bias[i, :, where] = f * img[i, :, where] * g

    @pl.loop(0, blocks)
    def _(i):
        for t in range(tiles):
            weight = weight_ref[i, t].astype(jnp.float32) * fidelity_scale
            fid[i, :, at(t)] = weight * (1 - mask_v[i, :, at(t)]).astype(jnp.float32)
            coefficients(i, at(t))
            value = img[i, :, at(t)]
            prim[i, :, at(t)] = value
            ext[i, :, at(t)] = value
            dual_r[i, :, at(t)] = jnp.zeros((BR, TW), jnp.float32)
            dual_c[i, :, at(t)] = jnp.zeros((BR, TW), jnp.float32)

    row_msg[0] = jnp.where(sub_w < HALF, img[0, :, pl.ds(0, width)], pltpu.roll(fid[0, :, pl.ds(0, width)], HALF, 0))
    row_msg[1] = jnp.where(
        sub_w >= HALF, img[last, :, pl.ds(0, width)], pltpu.roll(fid[last, :, pl.ds(0, width)], HALF, 0)
    )
    rows_here = blocks * BR
    for side, start in ((0, 0), (1, width - TW)):
        both = jnp.concatenate(
            [
                img[pl.ds(0, blocks), :, pl.ds(start, TW)].reshape(rows_here, TW),
                fid[pl.ds(0, blocks), :, pl.ds(start, TW)].reshape(rows_here, TW),
            ],
            axis=0,
        ).T
        col_msg[side] = both[:BR] if side == 0 else both[TW - BR :]

    def dual_update(e, e_right, e_below, dr, dc, no_row=None, no_col=None):
        grad_r = pltpu.roll(jnp.where(sub == 0, e_below, e), BR - 1, 0) - e
        grad_c = pltpu.roll(jnp.where(lane == 0, e_right, e), TW - 1, 1) - e
        if no_row is not None:
            grad_r = jnp.where(sub == no_row, 0.0, grad_r)
        if no_col is not None:
            grad_c = jnp.where(lane == no_col, 0.0, grad_c)
        trial_r, trial_c = dr + sigma_step * grad_r, dc + sigma_step * grad_c
        scale = jnp.minimum(1.0, tv_weight * lax.rsqrt(trial_r * trial_r + trial_c * trial_c))
        return trial_r * scale, trial_c * scale, jnp.sqrt(grad_r * grad_r + grad_c * grad_c)

    def primal_update(p, dr, dc, dr_above, dc_left, g, b):
        upper = pltpu.roll(jnp.where(sub == BR - 1, dr_above, dr), 1, 0)
        before = pltpu.roll(jnp.where(lane == TW - 1, dc_left, dc), 1, 1)
        return (p + tau_step * ((dr - upper) + (dc - before))) * g + b

    def loss(variation, f, misfit):
        return tv_weight * variation + 0.5 * f * (misfit * misfit)

    zero = jnp.zeros((BR, TW), jnp.float32)

    @pl.loop(0, ITERS)
    def _(step):
        partial = [zero, zero]
        for i in range(blocks):
            for t in range(tiles):
                e = ext[i, :, at(t)]
                dr, dc, variation = dual_update(
                    e, ext[i, :, at(min(t + 1, last_t))], ext[min(i + 1, last), :, at(t)],
                    dual_r[i, :, at(t)], dual_c[i, :, at(t)],
                )
                dual_r[i, :, at(t)] = dr
                dual_c[i, :, at(t)] = dc
                p = prim[i, :, at(t)]
                updated = primal_update(
                    p, dr, dc, dual_r[max(i - 1, 0), :, at(t)], dual_c[i, :, at(max(t - 1, 0))],
                    gain[i, :, at(t)], bias[i, :, at(t)],
                )
                ext[i, :, at(t)] = 2.0 * updated - p
                prim[i, :, at(t)] = updated
                term = loss(variation, fid[i, :, at(t)], updated - img[i, :, at(t)])
                if i in (0, last):
                    term = jnp.where(sub >= HALF if i == 0 else sub < HALF, term, 0.0)
                if t in (0, last_t):
                    term = jnp.where(lane >= TW // 2 if t == 0 else lane < TW // 2, term, 0.0)
                partial[t % 2] = partial[t % 2] + term
        acc[step] = partial[0] + partial[1]

    for i in range(blocks):
        for t in range(tiles):
            value = prim[i, :, at(t)]
            staged[2 * t, i] = value[:HALF]
            staged[2 * t + 1, i] = value[HALF:]

    pl.semaphore_wait(barrier, n_rows - 1 + n_cols - 1 + 4)

    first_tile, last_tile = pl.ds(0, TW), pl.ds(width - TW, TW)
    messages = (
        (row_msg.at[0], row_got.at[0], up, c),
        (row_msg.at[1], row_got.at[1], down, c),
        (col_msg.at[0], col_got.at[0], r, left),
        (col_msg.at[1], col_got.at[1], r, right),
        (row_msg.at[0, :, first_tile], corner_got.at[0], up, left),
        (row_msg.at[0, :, last_tile], corner_got.at[1], up, right),
        (row_msg.at[1, :, first_tile], corner_got.at[2], down, left),
        (row_msg.at[1, :, last_tile], corner_got.at[3], down, right),
    )
    halos = [
        pltpu.make_async_remote_copy(
            src_ref=src, dst_ref=dst, send_sem=halo_send.at[k], recv_sem=halo_recv.at[k],
            device_id=(row, col), device_id_type=MESH,
        )
        for k, (src, dst, row, col) in enumerate(messages)
    ]
    for k in (2, 3, 4, 5, 6, 7, 0, 1):
        halos[k].start()

    def spread_to(m, start, size):
        piece = pl.ds(start, size)
        return pltpu.make_async_remote_copy(
            src_ref=staged.at[m, piece], dst_ref=spread.at[r, piece], send_sem=send1, recv_sem=recv1,
            device_id=(m, c), device_id_type=MESH,
        )

    @pl.loop(1, n_rows)
    def _(j):
        m = lax.rem(r + j, n_rows)

        @pl.when((m >= 2) & (m < n_rows - 2))
        def _():
            spread_to(m, 1 - lax.rem(m, 2), last).start()

    for halo in halos:
        halo.wait_recv()

    below, above = row_got[0], row_got[1]
    img[blocks, :, pl.ds(0, width)] = jnp.where(sub_w < HALF, below, above)
    fid[blocks, :, pl.ds(0, width)] = pltpu.roll(jnp.where(sub_w < HALF, above, below), HALF, 0)
    sides = jnp.concatenate([col_got[0], jnp.zeros((TW - 2 * BR, TW), jnp.float32), col_got[1]], axis=0).T
    img[pl.ds(0, blocks), :, pl.ds(width, TW)] = sides[:rows_here].reshape(blocks, BR, TW)
    fid[pl.ds(0, blocks), :, pl.ds(width, TW)] = sides[rows_here:].reshape(blocks, BR, TW)
    low = jnp.where(lane < TW // 2, corner_got[0], corner_got[1])
    high = jnp.where(lane < TW // 2, corner_got[2], corner_got[3])
    img[blocks, :, pl.ds(width, TW)] = jnp.where(sub < HALF, low, high)
    fid[blocks, :, pl.ds(width, TW)] = pltpu.roll(jnp.where(sub < HALF, high, low), HALF, 0)

    coefficients(blocks, pl.ds(0, ring))
    for i in range(blocks):
        coefficients(i, at(tiles))

    rows_of, cols_of = (last, blocks, 0), (last_t, tiles, 0)
    no_rows = (jnp.where(r == n_rows - 1, BR - 1, BR), jnp.where(r == 0, BR - 1, BR), None)
    no_cols = (jnp.where(c == n_cols - 1, TW - 1, TW), jnp.where(c == 0, TW - 1, TW), None)

    for k in range(3):
        for t in range(tiles):
            value = img[rows_of[k], :, at(t)]
            strip_prim[k, :, at(t)] = value
            strip_ext[k, :, at(t)] = value
            strip_r[k, :, at(t)] = zero
            strip_c[k, :, at(t)] = zero
    for i in range(blocks + 1):
        for k in range(3):
            value = img[i, :, at(cols_of[k])]
            side_prim[i, :, at(k)] = value
            side_ext[i, :, at(k)] = value
            side_r[i, :, at(k)] = zero
            side_c[i, :, at(k)] = zero

    @pl.loop(0, ITERS)
    def _(step):
        partial = acc[step]
        for t in range(tiles):
            e = [strip_ext[k, :, at(t)] for k in range(3)]
            duals = []
            for k in range(3):
                duals.append(
                    dual_update(
                        e[k], strip_ext[k, :, at(min(t + 1, last_t))], e[(k + 1) % 3],
                        strip_r[k, :, at(t)], strip_c[k, :, at(t)], no_row=no_rows[k],
                    )
                )
            for k in range(3):
                dr, dc, variation = duals[k]
                strip_r[k, :, at(t)] = dr
                strip_c[k, :, at(t)] = dc
                p = strip_prim[k, :, at(t)]
                i = rows_of[k]
                updated = primal_update(
                    p, dr, dc, duals[(k + 2) % 3][0], strip_c[k, :, at(max(t - 1, 0))],
                    gain[i, :, at(t)], bias[i, :, at(t)],
                )
                strip_ext[k, :, at(t)] = 2.0 * updated - p
                strip_prim[k, :, at(t)] = updated
                if k != 1:
                    term = loss(variation, fid[i, :, at(t)], updated - img[i, :, at(t)])
                    term = jnp.where(sub < HALF if k == 2 else sub >= HALF, term, 0.0)
                    if t in (0, last_t):
                        term = jnp.where(lane >= TW // 2 if t == 0 else lane < TW // 2, term, 0.0)
                    partial = partial + term
        variations = {}
        e = [[side_ext[i, :, at(k)] for k in range(3)] for i in range(blocks + 1)]
        for i in range(blocks + 1):
            no_row = no_rows[0] if i == last else no_rows[1] if i == blocks else None
            for k in range(3):
                dr, dc, variations[i, k] = dual_update(
                    e[i][k], e[i][(k + 1) % 3], e[(i + 1) % (blocks + 1)][k],
                    side_r[i, :, at(k)], side_c[i, :, at(k)], no_row=no_row, no_col=no_cols[k],
                )
                side_r[i, :, at(k)] = dr
                side_c[i, :, at(k)] = dc
        for i in range(blocks + 1):
            for k in range(3):
                t = cols_of[k]
                p = side_prim[i, :, at(k)]
                updated = primal_update(
                    p, side_r[i, :, at(k)], side_c[i, :, at(k)], side_r[(i + blocks) % (blocks + 1), :, at(k)],
                    side_c[i, :, at((k + 2) % 3)], gain[i, :, at(t)], bias[i, :, at(t)],
                )
                side_ext[i, :, at(k)] = 2.0 * updated - p
                side_prim[i, :, at(k)] = updated
                if k != 1 and i < blocks:
                    term = loss(variations[i, k], fid[i, :, at(t)], updated - img[i, :, at(t)])
                    partial = partial + jnp.where(lane < TW // 2 if k == 2 else lane >= TW // 2, term, 0.0)
        acc[step] = partial

    for t in range(1, last_t):
        staged[2 * t, 0] = strip_prim[2, :HALF, at(t)]
        staged[2 * t + 1, last] = strip_prim[0, HALF:, at(t)]
    for k, t in ((2, 0), (0, last_t)):
        for i in range(blocks):
            value = prim[i, :, at(t)]
            if i == 0:
                value = jnp.where(sub < HALF, strip_prim[2, :, at(t)], value)
            if i == last:
                value = jnp.where(sub >= HALF, strip_prim[0, :, at(t)], value)
            value = jnp.where(lane < TW // 2 if k == 2 else lane >= TW // 2, side_prim[i, :, at(k)], value)
            staged[2 * t, i] = value[:HALF]
            staged[2 * t + 1, i] = value[HALF:]

    lane_1 = lax.broadcasted_iota(jnp.int32, (1, TW), 1)
    sums = jnp.zeros((1, TW), jnp.float32)
    for step in range(ITERS):
        line = jnp.sum(acc[step], axis=0, keepdims=True)
        sums = jnp.where(lane_1 == step, jnp.sum(line, axis=1, keepdims=True), sums)
    part_src[...] = sums
    part_rows[r] = sums

    def part_to(m):
        return pltpu.make_async_remote_copy(
            src_ref=part_src, dst_ref=part_rows.at[r], send_sem=psend, recv_sem=precv,
            device_id=(m, c), device_id_type=MESH,
        )

    @pl.loop(1, n_rows)
    def _(j):
        m = lax.rem(r + j, n_rows)
        inner = (m >= 2) & (m < n_rows - 2)

        @pl.when(inner)
        def _():
            spread_to(m, last * lax.rem(m, 2), 1).start()

        @pl.when(jnp.logical_not(inner))
        def _():
            spread_to(m, 0, blocks).start()

    @pl.loop(1, n_rows)
    def _(j):
        part_to(lax.rem(r + j, n_rows)).start()

    spread[r] = staged[r]
    to_scalars.wait()
    peers = pl.ds(0, n_rows - 1)
    all_spread = pltpu.make_async_remote_copy(
        src_ref=staged.at[peers], dst_ref=spread.at[peers], send_sem=send1, recv_sem=recv1,
        device_id=(up, c), device_id_type=MESH,
    )
    all_spread.wait_recv()

    def collect_to(d):
        return pltpu.make_async_remote_copy(
            src_ref=sorted_.at[d], dst_ref=gathered.at[r], send_sem=send2, recv_sem=recv2,
            device_id=(d, c), device_id_type=MESH,
        )

    def sort_for(d):
        for k in range(blocks):
            b = order_s[0, d * blocks + k]
            sorted_[d, k] = spread[b // blocks, lax.rem(b, blocks)]

    sort_for(lax.rem(r + 1, n_rows))

    @pl.loop(2, n_rows)
    def _(j):
        sort_for(lax.rem(r + j, n_rows))
        collect_to(lax.rem(r + j - 1, n_rows)).start()

    sort_for(r)
    collect_to(up).start()
    gathered[r] = sorted_[r]

    all_parts = pltpu.make_async_remote_copy(
        src_ref=part_rows.at[peers], dst_ref=part_rows.at[peers], send_sem=psend, recv_sem=precv,
        device_id=(up, c), device_id_type=MESH,
    )
    all_parts.wait_recv()
    here = part_rows[0]
    for s in range(1, n_rows):
        here = here + part_rows[s]
    part_src_c[...] = here
    part_cols[c] = here

    def part_across(col):
        return pltpu.make_async_remote_copy(
            src_ref=part_src_c, dst_ref=part_cols.at[c], send_sem=csend, recv_sem=crecv,
            device_id=(r, col), device_id_type=MESH,
        )

    @pl.loop(1, n_cols)
    def _(j):
        part_across(lax.rem(c + j, n_cols)).start()

    col_peers = pl.ds(0, n_cols - 1)
    all_cols = pltpu.make_async_remote_copy(
        src_ref=part_cols.at[col_peers], dst_ref=part_cols.at[col_peers], send_sem=csend, recv_sem=crecv,
        device_id=(r, left), device_id_type=MESH,
    )
    all_cols.wait_recv()
    everywhere = part_cols[0]
    for s in range(1, n_cols):
        everywhere = everywhere + part_cols[s]
    for step in range(ITERS):
        objective_ref[step] = jnp.sum(jnp.where(lane_1 == step, everywhere, 0.0)) / pixel_total

    all_collected = pltpu.make_async_remote_copy(
        src_ref=sorted_.at[peers], dst_ref=gathered.at[peers], send_sem=send2, recv_sem=recv2,
        device_id=(up, c), device_id_type=MESH,
    )
    all_collected.wait_recv()

    @pl.loop(0, blocks)
    def _(k):
        for t in range(tiles):
            out_v[k, :, pl.ds(t * TW, TW)] = jnp.concatenate([gathered[2 * t, k], gathered[2 * t + 1, k]], axis=0)

    store = pltpu.make_async_copy(out_v, out_hbm, out_sem)
    store.start()
    for halo in halos:
        halo.wait_send()
    all_spread.wait_send()
    all_parts.wait_send()
    all_cols.wait_send()
    all_collected.wait_send()
    store.wait()


def per_device(n_rows, n_cols, image, cloud_mask, tile_weight, owner):
    rows_here, width = image.shape
    blocks = rows_here // BR
    tiles = width // TW
    pixel_total = float(n_rows * n_cols * rows_here * width)
    f32 = jnp.float32
    ringed = pltpu.VMEM((blocks + 1, BR, width + TW), f32)
    pieces = pltpu.VMEM((n_rows, blocks, HALF, TW), f32)
    dma = pltpu.SemaphoreType.DMA
    scratch = (
        [ringed] * 4
        + [pltpu.VMEM((blocks, BR, width), f32)] * 4
        + [pltpu.VMEM((3, BR, width), f32)] * 4
        + [pltpu.VMEM((blocks + 1, BR, 3 * TW), f32)] * 4
        + [
            pltpu.VMEM((blocks, BR, width), jnp.int32),
            pltpu.VMEM((2, BR, width), f32),
            pltpu.VMEM((2, BR, width), f32),
            pltpu.VMEM((2, BR, TW), f32),
            pltpu.VMEM((2, BR, TW), f32),
            pltpu.VMEM((4, BR, TW), f32),
        ]
        + [pieces] * 4
        + [
            pltpu.VMEM((blocks, BR, width), f32),
            pltpu.VMEM((1, n_rows * blocks), jnp.int32),
            pltpu.SMEM((1, n_rows * blocks), jnp.int32),
            pltpu.VMEM((ITERS, BR, TW), f32),
            pltpu.VMEM((1, TW), f32),
            pltpu.VMEM((n_rows, 1, TW), f32),
            pltpu.VMEM((1, TW), f32),
            pltpu.VMEM((n_cols, 1, TW), f32),
            dma((2,)), dma, dma((8,)), dma((8,)),
            dma, dma, dma, dma, dma, dma, dma, dma, dma,
        ]
    )
    vmem, smem, hbm = (pl.BlockSpec(memory_space=s) for s in (pltpu.VMEM, pltpu.SMEM, pl.ANY))
    out, objective = pl.pallas_call(
        functools.partial(kernel, n_rows, n_cols, blocks, tiles, pixel_total),
        out_shape=(
            jax.ShapeDtypeStruct((blocks, BR, width), f32),
            jax.ShapeDtypeStruct((ITERS,), f32),
        ),
        in_specs=[hbm, hbm, smem, vmem],
        out_specs=(hbm, smem),
        scratch_shapes=scratch,
        compiler_params=pltpu.CompilerParams(collective_id=0, has_side_effects=True),
    )(
        image.reshape(blocks, BR, width),
        cloud_mask.reshape(blocks, BR, width),
        tile_weight,
        owner.reshape(1, -1),
    )
    return out.reshape(rows_here, width), objective


def solution(mesh):
    placed = (P("rows", "cols"), P("rows", "cols"), P("rows", "cols"), P())
    return jax.shard_map(
        functools.partial(per_device, mesh.shape["rows"], mesh.shape["cols"]),
        mesh=mesh, in_specs=placed, out_specs=(P("rows", "cols"), P()), check_vma=False,
    )
```

```python
import functools

import jax
import jax.numpy as jnp
from jax import lax
from jax.experimental import pallas as pl
from jax.experimental.pallas import tpu as pltpu
from jax.sharding import PartitionSpec as P

BR = 8
TW = 128
ITERS = 3
HALF = 4

fidelity_scale = 0.25
tau_step = 0.35
sigma_step = 0.35
tv_weight = 0.3

MESH = pl.DeviceIdType.MESH


def kernel(
    n_rows, n_cols, blocks, tiles, pixel_total,
    image_hbm, mask_hbm, weight_ref, owner_ref,
    gathered, objective_ref,
    img, fid, gain, bias, prim, ext, dual_r, dual_c,
    strip_prim, strip_ext, strip_r, strip_c, side_prim, side_ext, side_r, side_c, mask_v,
    row_msg, row_got, col_msg, col_got, corner_got,
    staged, spread, sorted_,
    order_v, order_s, acc, part_src, part_rows, part_src_c, part_cols,
    load_sem, order_sem, halo_send, halo_recv,
    send1, recv1, send2, recv2, psend, precv, csend, crecv, ready,
):
    width = tiles * TW
    ring = width + TW
    r = lax.axis_index("rows")
    c = lax.axis_index("cols")
    up, down = lax.rem(r + n_rows - 1, n_rows), lax.rem(r + 1, n_rows)
    left, right = lax.rem(c + n_cols - 1, n_cols), lax.rem(c + 1, n_cols)

    load_image = pltpu.make_async_copy(image_hbm, img.at[pl.ds(0, blocks), :, pl.ds(0, width)], load_sem.at[0])
    load_mask = pltpu.make_async_copy(mask_hbm, mask_v, load_sem.at[1])
    load_image.start()
    load_mask.start()

    span = 4
    depth = n_rows // span

    def peer(j):
        near = lax.rem(lax.rem(r, depth) + lax.div(j, span), depth)
        return lax.rem(lax.div(r, depth) + lax.rem(j, span), span) * depth + near

    barrier = pltpu.get_barrier_semaphore()
    odd = lax.rem(c, 2) == 1
    even = jnp.logical_not(odd)
    opposite = n_cols // 2

    def across(signal):
        for n in range(opposite):
            signal(r, lax.rem(c + 2 * n + 1, n_cols))
        for row in (up, down):
            for col in (left, right):
                signal(row, col)

    def greet(row, col):
        pl.semaphore_signal(barrier, inc=1, device_id=(row, col), device_id_type=MESH)

    def answer(row, col):
        pl.semaphore_signal(ready, inc=1, device_id=(row, col), device_id_type=MESH)

    @pl.when(even)
    def _():
        across(greet)

    for n in range(1, opposite):
        greet(r, lax.rem(c + 2 * n, n_cols))

    @pl.loop(1, n_rows)
    def _(j):
        greet(peer(j), c)

    total = n_rows * blocks
    own = jnp.broadcast_to(owner_ref[...], (total, total))
    before = lax.broadcasted_iota(jnp.int32, (total, total), 0)
    after = lax.broadcasted_iota(jnp.int32, (total, total), 1)
    same = (own == own.T) & (before < after)
    rank = jnp.sum(jnp.where(same, 1, 0), axis=0, keepdims=True)
    place = jnp.broadcast_to(owner_ref[...] * blocks + rank, (total, total)).T
    order_v[...] = jnp.sum(jnp.where(place == after, before, 0), axis=0, keepdims=True)
    to_scalars = pltpu.make_async_copy(order_v, order_s, order_sem)
    to_scalars.start()

    load_image.wait()
    load_mask.wait()

    sub = lax.broadcasted_iota(jnp.int32, (BR, TW), 0)
    lane = lax.broadcasted_iota(jnp.int32, (BR, TW), 1)
    sub_w = lax.broadcasted_iota(jnp.int32, (BR, width), 0)
    last, last_t = blocks - 1, tiles - 1

    def at(t):
        return pl.ds(t * TW if isinstance(t, int) else pl.multiple_of(t * TW, TW), TW)

    def coefficients(i, where):
        f = fid[i, :, where] * tau_step
        g = 1.0 / (1.0 + f)
        gain[i, :, where] = g
        bias[i, :, where] = f * img[i, :, where] * g

    @pl.loop(0, blocks)
    def _(i):
        for t in range(tiles):
            weight = weight_ref[i, t].astype(jnp.float32) * fidelity_scale
            fid[i, :, at(t)] = weight * (1 - mask_v[i, :, at(t)]).astype(jnp.float32)
            coefficients(i, at(t))
            value = img[i, :, at(t)]
            prim[i, :, at(t)] = value
            ext[i, :, at(t)] = value
            dual_r[i, :, at(t)] = jnp.zeros((BR, TW), jnp.float32)
            dual_c[i, :, at(t)] = jnp.zeros((BR, TW), jnp.float32)

    row_msg[0] = jnp.where(sub_w < HALF, img[0, :, pl.ds(0, width)], pltpu.roll(fid[0, :, pl.ds(0, width)], HALF, 0))
    row_msg[1] = jnp.where(
        sub_w >= HALF, img[last, :, pl.ds(0, width)], pltpu.roll(fid[last, :, pl.ds(0, width)], HALF, 0)
    )
    rows_here = blocks * BR
    for side, start in ((0, 0), (1, width - TW)):
        both = jnp.concatenate(
            [
                img[pl.ds(0, blocks), :, pl.ds(start, TW)].reshape(rows_here, TW),
                fid[pl.ds(0, blocks), :, pl.ds(start, TW)].reshape(rows_here, TW),
            ],
            axis=0,
        ).T
        col_msg[side] = both[:BR] if side == 0 else both[TW - BR :]

    first_tile, last_tile = pl.ds(0, TW), pl.ds(width - TW, TW)
    messages = (
        (row_msg.at[0], row_got.at[0], up, c),
        (row_msg.at[1], row_got.at[1], down, c),
        (col_msg.at[0], col_got.at[0], r, left),
        (col_msg.at[1], col_got.at[1], r, right),
        (row_msg.at[0, :, first_tile], corner_got.at[0], up, left),
        (row_msg.at[0, :, last_tile], corner_got.at[1], up, right),
        (row_msg.at[1, :, first_tile], corner_got.at[2], down, left),
        (row_msg.at[1, :, last_tile], corner_got.at[3], down, right),
    )
    halos = [
        pltpu.make_async_remote_copy(
            src_ref=src, dst_ref=dst, send_sem=halo_send.at[k], recv_sem=halo_recv.at[k],
            device_id=(row, col), device_id_type=MESH,
        )
        for k, (src, dst, row, col) in enumerate(messages)
    ]

    @pl.when(odd)
    def _():
        pl.semaphore_wait(barrier, n_rows - 1 + n_cols - 1 + 4)
        across(answer)
        for halo in halos[2:] + halos[:2]:
            halo.start()

    def dual_update(e, e_right, e_below, dr, dc, no_row=None, no_col=None):
        grad_r = pltpu.roll(jnp.where(sub == 0, e_below, e), BR - 1, 0) - e
        grad_c = pltpu.roll(jnp.where(lane == 0, e_right, e), TW - 1, 1) - e
        if no_row is not None:
            grad_r = jnp.where(sub == no_row, 0.0, grad_r)
        if no_col is not None:
            grad_c = jnp.where(lane == no_col, 0.0, grad_c)
        trial_r, trial_c = dr + sigma_step * grad_r, dc + sigma_step * grad_c
        scale = jnp.minimum(1.0, tv_weight * lax.rsqrt(trial_r * trial_r + trial_c * trial_c))
        return trial_r * scale, trial_c * scale, jnp.sqrt(grad_r * grad_r + grad_c * grad_c)

    def primal_update(p, dr, dc, dr_above, dc_left, g, b):
        upper = pltpu.roll(jnp.where(sub == BR - 1, dr_above, dr), 1, 0)
        before = pltpu.roll(jnp.where(lane == TW - 1, dc_left, dc), 1, 1)
        return (p + tau_step * ((dr - upper) + (dc - before))) * g + b

    def loss(variation, f, misfit):
        return tv_weight * variation + 0.5 * f * (misfit * misfit)

    zero = jnp.zeros((BR, TW), jnp.float32)

    @pl.loop(0, ITERS)
    def _(step):
        partial = [zero, zero]
        for i in range(blocks):
            for t in range(tiles):
                e = ext[i, :, at(t)]
                dr, dc, variation = dual_update(
                    e, ext[i, :, at(min(t + 1, last_t))], ext[min(i + 1, last), :, at(t)],
                    dual_r[i, :, at(t)], dual_c[i, :, at(t)],
                )
                dual_r[i, :, at(t)] = dr
                dual_c[i, :, at(t)] = dc
                p = prim[i, :, at(t)]
                updated = primal_update(
                    p, dr, dc, dual_r[max(i - 1, 0), :, at(t)], dual_c[i, :, at(max(t - 1, 0))],
                    gain[i, :, at(t)], bias[i, :, at(t)],
                )
                ext[i, :, at(t)] = 2.0 * updated - p
                prim[i, :, at(t)] = updated
                term = loss(variation, fid[i, :, at(t)], updated - img[i, :, at(t)])
                if i in (0, last):
                    term = jnp.where(sub >= HALF if i == 0 else sub < HALF, term, 0.0)
                if t in (0, last_t):
                    term = jnp.where(lane >= TW // 2 if t == 0 else lane < TW // 2, term, 0.0)
                partial[t % 2] = partial[t % 2] + term
        acc[step] = partial[0] + partial[1]

    for i in range(blocks):
        for t in range(tiles):
            value = prim[i, :, at(t)]
            staged[2 * t, i] = value[:HALF]
            staged[2 * t + 1, i] = value[HALF:]

    def spread_to(m, start, size):
        piece = pl.ds(start, size)
        return pltpu.make_async_remote_copy(
            src_ref=staged.at[m, piece], dst_ref=spread.at[r, piece], send_sem=send1, recv_sem=recv1,
            device_id=(m, c), device_id_type=MESH,
        )

    @pl.when(even)
    def _():
        pl.semaphore_wait(barrier, n_rows - 1 + opposite - 1)
        for halo in halos[:2]:
            halo.start()

    @pl.loop(1, n_rows)
    def _(j):
        m = peer(j)

        @pl.when((m >= 2) & (m < n_rows - 2))
        def _():
            spread_to(m, 1 - lax.rem(m, 2), last).start()

    @pl.when(even)
    def _():
        pl.semaphore_wait(ready, opposite + 4)
        for halo in halos[2:]:
            halo.start()

    for halo in halos:
        halo.wait_recv()

    below, above = row_got[0], row_got[1]
    img[blocks, :, pl.ds(0, width)] = jnp.where(sub_w < HALF, below, above)
    fid[blocks, :, pl.ds(0, width)] = pltpu.roll(jnp.where(sub_w < HALF, above, below), HALF, 0)
    sides = jnp.concatenate([col_got[0], jnp.zeros((TW - 2 * BR, TW), jnp.float32), col_got[1]], axis=0).T
    img[pl.ds(0, blocks), :, pl.ds(width, TW)] = sides[:rows_here].reshape(blocks, BR, TW)
    fid[pl.ds(0, blocks), :, pl.ds(width, TW)] = sides[rows_here:].reshape(blocks, BR, TW)
    low = jnp.where(lane < TW // 2, corner_got[0], corner_got[1])
    high = jnp.where(lane < TW // 2, corner_got[2], corner_got[3])
    img[blocks, :, pl.ds(width, TW)] = jnp.where(sub < HALF, low, high)
    fid[blocks, :, pl.ds(width, TW)] = pltpu.roll(jnp.where(sub < HALF, high, low), HALF, 0)

    coefficients(blocks, pl.ds(0, ring))
    for i in range(blocks):
        coefficients(i, at(tiles))

    rows_of, cols_of = (last, blocks, 0), (last_t, tiles, 0)
    no_rows = (jnp.where(r == n_rows - 1, BR - 1, BR), jnp.where(r == 0, BR - 1, BR), None)
    no_cols = (jnp.where(c == n_cols - 1, TW - 1, TW), jnp.where(c == 0, TW - 1, TW), None)

    for k in range(3):
        for t in range(tiles):
            value = img[rows_of[k], :, at(t)]
            strip_prim[k, :, at(t)] = value
            strip_ext[k, :, at(t)] = value
            strip_r[k, :, at(t)] = zero
            strip_c[k, :, at(t)] = zero
    for i in range(blocks + 1):
        for k in range(3):
            value = img[i, :, at(cols_of[k])]
            side_prim[i, :, at(k)] = value
            side_ext[i, :, at(k)] = value
            side_r[i, :, at(k)] = zero
            side_c[i, :, at(k)] = zero

    @pl.loop(0, ITERS)
    def _(step):
        partial = acc[step]
        for t in range(tiles):
            e = [strip_ext[k, :, at(t)] for k in range(3)]
            duals = []
            for k in range(3):
                duals.append(
                    dual_update(
                        e[k], strip_ext[k, :, at(min(t + 1, last_t))], e[(k + 1) % 3],
                        strip_r[k, :, at(t)], strip_c[k, :, at(t)], no_row=no_rows[k],
                    )
                )
            for k in range(3):
                dr, dc, variation = duals[k]
                strip_r[k, :, at(t)] = dr
                strip_c[k, :, at(t)] = dc
                p = strip_prim[k, :, at(t)]
                i = rows_of[k]
                updated = primal_update(
                    p, dr, dc, duals[(k + 2) % 3][0], strip_c[k, :, at(max(t - 1, 0))],
                    gain[i, :, at(t)], bias[i, :, at(t)],
                )
                strip_ext[k, :, at(t)] = 2.0 * updated - p
                strip_prim[k, :, at(t)] = updated
                if k != 1:
                    term = loss(variation, fid[i, :, at(t)], updated - img[i, :, at(t)])
                    term = jnp.where(sub < HALF if k == 2 else sub >= HALF, term, 0.0)
                    if t in (0, last_t):
                        term = jnp.where(lane >= TW // 2 if t == 0 else lane < TW // 2, term, 0.0)
                    partial = partial + term
        variations = {}
        e = [[side_ext[i, :, at(k)] for k in range(3)] for i in range(blocks + 1)]
        for i in range(blocks + 1):
            no_row = no_rows[0] if i == last else no_rows[1] if i == blocks else None
            for k in range(3):
                dr, dc, variations[i, k] = dual_update(
                    e[i][k], e[i][(k + 1) % 3], e[(i + 1) % (blocks + 1)][k],
                    side_r[i, :, at(k)], side_c[i, :, at(k)], no_row=no_row, no_col=no_cols[k],
                )
                side_r[i, :, at(k)] = dr
                side_c[i, :, at(k)] = dc
        for i in range(blocks + 1):
            for k in range(3):
                t = cols_of[k]
                p = side_prim[i, :, at(k)]
                updated = primal_update(
                    p, side_r[i, :, at(k)], side_c[i, :, at(k)], side_r[(i + blocks) % (blocks + 1), :, at(k)],
                    side_c[i, :, at((k + 2) % 3)], gain[i, :, at(t)], bias[i, :, at(t)],
                )
                side_ext[i, :, at(k)] = 2.0 * updated - p
                side_prim[i, :, at(k)] = updated
                if k != 1 and i < blocks:
                    term = loss(variations[i, k], fid[i, :, at(t)], updated - img[i, :, at(t)])
                    partial = partial + jnp.where(lane < TW // 2 if k == 2 else lane >= TW // 2, term, 0.0)
        acc[step] = partial

    for t in range(1, last_t):
        staged[2 * t, 0] = strip_prim[2, :HALF, at(t)]
        staged[2 * t + 1, last] = strip_prim[0, HALF:, at(t)]
    for k, t in ((2, 0), (0, last_t)):
        for i in range(blocks):
            value = prim[i, :, at(t)]
            if i == 0:
                value = jnp.where(sub < HALF, strip_prim[2, :, at(t)], value)
            if i == last:
                value = jnp.where(sub >= HALF, strip_prim[0, :, at(t)], value)
            value = jnp.where(lane < TW // 2 if k == 2 else lane >= TW // 2, side_prim[i, :, at(k)], value)
            staged[2 * t, i] = value[:HALF]
            staged[2 * t + 1, i] = value[HALF:]

    lane_1 = lax.broadcasted_iota(jnp.int32, (1, TW), 1)
    sums = jnp.zeros((1, TW), jnp.float32)
    for step in range(ITERS):
        line = jnp.sum(acc[step], axis=0, keepdims=True)
        sums = jnp.where(lane_1 == step, jnp.sum(line, axis=1, keepdims=True), sums)
    part_src[...] = sums
    part_rows[r] = sums

    def part_to(m):
        return pltpu.make_async_remote_copy(
            src_ref=part_src, dst_ref=part_rows.at[r], send_sem=psend, recv_sem=precv,
            device_id=(m, c), device_id_type=MESH,
        )

    @pl.loop(1, n_rows)
    def _(j):
        part_to(peer(j)).start()

    @pl.loop(1, n_rows)
    def _(j):
        m = peer(j)
        inner = (m >= 2) & (m < n_rows - 2)

        @pl.when(inner)
        def _():
            spread_to(m, last * lax.rem(m, 2), 1).start()

        @pl.when(jnp.logical_not(inner))
        def _():
            spread_to(m, 0, blocks).start()

    spread[r] = staged[r]
    to_scalars.wait()
    peers = pl.ds(0, n_rows - 1)
    all_spread = pltpu.make_async_remote_copy(
        src_ref=staged.at[peers], dst_ref=spread.at[peers], send_sem=send1, recv_sem=recv1,
        device_id=(up, c), device_id_type=MESH,
    )
    all_spread.wait_recv()

    all_parts = pltpu.make_async_remote_copy(
        src_ref=part_rows.at[peers], dst_ref=part_rows.at[peers], send_sem=psend, recv_sem=precv,
        device_id=(up, c), device_id_type=MESH,
    )
    all_parts.wait_recv()
    here = part_rows[0]
    for s in range(1, n_rows):
        here = here + part_rows[s]
    part_src_c[...] = here
    part_cols[c] = here

    def part_across(col):
        return pltpu.make_async_remote_copy(
            src_ref=part_src_c, dst_ref=part_cols.at[c], send_sem=csend, recv_sem=crecv,
            device_id=(r, col), device_id_type=MESH,
        )

    @pl.loop(1, n_cols)
    def _(j):
        part_across(lax.rem(c + j, n_cols)).start()

    def collect_to(d):
        return pltpu.make_async_remote_copy(
            src_ref=sorted_.at[d], dst_ref=gathered.at[r], send_sem=send2, recv_sem=recv2,
            device_id=(d, c), device_id_type=MESH,
        )

    def sort_for(d):
        for k in range(blocks):
            b = order_s[0, d * blocks + k]
            sorted_[d, k] = spread[b // blocks, lax.rem(b, blocks)]

    sort_for(peer(1))

    @pl.loop(2, n_rows)
    def _(j):
        sort_for(peer(j))
        collect_to(peer(j - 1)).start()

    sort_for(r)
    collect_to(peer(n_rows - 1)).start()
    gathered[r] = sorted_[r]

    col_peers = pl.ds(0, n_cols - 1)
    all_cols = pltpu.make_async_remote_copy(
        src_ref=part_cols.at[col_peers], dst_ref=part_cols.at[col_peers], send_sem=csend, recv_sem=crecv,
        device_id=(r, left), device_id_type=MESH,
    )
    all_cols.wait_recv()
    everywhere = part_cols[0]
    for s in range(1, n_cols):
        everywhere = everywhere + part_cols[s]
    objective_ref[...] = everywhere / pixel_total

    all_collected = pltpu.make_async_remote_copy(
        src_ref=sorted_.at[peers], dst_ref=gathered.at[peers], send_sem=send2, recv_sem=recv2,
        device_id=(up, c), device_id_type=MESH,
    )
    all_collected.wait_recv()

    for halo in halos:
        halo.wait_send()
    all_spread.wait_send()
    all_parts.wait_send()
    all_cols.wait_send()
    all_collected.wait_send()


def assemble(pieces, row, out_hbm, objective, out, sems):
    blocks, _, width = out.shape
    stores = [pltpu.make_async_copy(out.at[k], out_hbm.at[k], sems.at[k]) for k in range(blocks)]
    for k in range(blocks):
        for t in range(width // TW):
            out[k, :, pl.ds(t * TW, TW)] = jnp.concatenate([pieces[2 * t, k], pieces[2 * t + 1, k]], axis=0)
        stores[k].start()
    lanes = lax.broadcasted_iota(jnp.int32, (1, TW), 1)
    for step in range(ITERS):
        objective[step] = jnp.sum(jnp.where(lanes == step, row[...], 0.0))
    for store in stores:
        store.wait()


def per_device(n_rows, n_cols, image, cloud_mask, tile_weight, owner):
    rows_here, width = image.shape
    blocks = rows_here // BR
    tiles = width // TW
    pixel_total = float(n_rows * n_cols * rows_here * width)
    f32 = jnp.float32
    ringed = pltpu.VMEM((blocks + 1, BR, width + TW), f32)
    pieces = pltpu.VMEM((n_rows, blocks, HALF, TW), f32)
    dma = pltpu.SemaphoreType.DMA
    scratch = (
        [ringed] * 4
        + [pltpu.VMEM((blocks, BR, width), f32)] * 4
        + [pltpu.VMEM((3, BR, width), f32)] * 4
        + [pltpu.VMEM((blocks + 1, BR, 3 * TW), f32)] * 4
        + [
            pltpu.VMEM((blocks, BR, width), jnp.int32),
            pltpu.VMEM((2, BR, width), f32),
            pltpu.VMEM((2, BR, width), f32),
            pltpu.VMEM((2, BR, TW), f32),
            pltpu.VMEM((2, BR, TW), f32),
            pltpu.VMEM((4, BR, TW), f32),
        ]
        + [pieces] * 3
        + [
            pltpu.VMEM((1, n_rows * blocks), jnp.int32),
            pltpu.SMEM((1, n_rows * blocks), jnp.int32),
            pltpu.VMEM((ITERS, BR, TW), f32),
            pltpu.VMEM((1, TW), f32),
            pltpu.VMEM((n_rows, 1, TW), f32),
            pltpu.VMEM((1, TW), f32),
            pltpu.VMEM((n_cols, 1, TW), f32),
            dma((2,)), dma, dma((8,)), dma((8,)),
            dma, dma, dma, dma, dma, dma, dma, dma,
            pltpu.SemaphoreType.REGULAR,
        ]
    )
    vmem, smem, hbm = (pl.BlockSpec(memory_space=s) for s in (pltpu.VMEM, pltpu.SMEM, pl.ANY))
    received, row = pl.pallas_call(
        functools.partial(kernel, n_rows, n_cols, blocks, tiles, pixel_total),
        out_shape=(
            pltpu.VMEM((n_rows, blocks, HALF, TW), f32),
            pltpu.VMEM((1, TW), f32),
        ),
        in_specs=[hbm, hbm, smem, vmem],
        out_specs=(vmem, vmem),
        scratch_shapes=scratch,
        compiler_params=pltpu.CompilerParams(collective_id=0, has_side_effects=True),
    )(
        image.reshape(blocks, BR, width),
        cloud_mask.reshape(blocks, BR, width),
        tile_weight,
        owner.reshape(1, -1),
    )
    out, objective = pl.pallas_call(
        assemble,
        out_shape=(jax.ShapeDtypeStruct((blocks, BR, width), f32), jax.ShapeDtypeStruct((ITERS,), f32)),
        in_specs=[vmem, vmem],
        out_specs=(hbm, smem),
        scratch_shapes=[pltpu.VMEM((blocks, BR, width), f32), dma((blocks,))],
    )(pltpu.with_memory_space_constraint(received, pltpu.VMEM), pltpu.with_memory_space_constraint(row, pltpu.VMEM))
    return out.reshape(rows_here, width), objective


def solution(mesh):
    placed = (P("rows", "cols"), P("rows", "cols"), P("rows", "cols"), P())
    return jax.shard_map(
        functools.partial(per_device, mesh.shape["rows"], mesh.shape["cols"]),
        mesh=mesh, in_specs=placed, out_specs=(P("rows", "cols"), P()), check_vma=False,
    )
```

```python
import functools

import jax
import jax.numpy as jnp
from jax import lax
from jax.experimental import pallas as pl
from jax.experimental.pallas import tpu as pltpu
from jax.sharding import PartitionSpec as P

BR = 8
TW = 128
ITERS = 3
HALF = 4
PAIR = 2

fidelity_scale = 0.25
tau_step = 0.35
sigma_step = 0.35
tv_weight = 0.3

MESH = pl.DeviceIdType.MESH


def kernel(
    n_rows, n_cols, blocks, tiles, pixel_total,
    image_hbm, mask_hbm, weight_ref, owner_ref,
    gathered, edge_gathered, objective_ref,
    img, fid, gain, bias, prim, ext, dual_r, dual_c,
    strip_prim, strip_ext, strip_r, strip_c, side_prim, side_ext, side_r, side_c, mask_v,
    row_msg, row_got, col_msg, col_got, corner_got,
    staged, spread_0, spread_1, sorted_, edge_staged, edge_spread, edge_sorted,
    order_v, order_s, acc, part_src, part_rows, part_src_c, part_cols,
    load_sem, order_sem, halo_send, halo_recv,
    send1, recv1, send2, recv2, psend, precv, csend, crecv, esend1, erecv1, esend2, erecv2, ready,
):
    spread = (spread_0, spread_1)
    width = tiles * TW
    ring = width + TW
    r = lax.axis_index("rows")
    c = lax.axis_index("cols")
    up, down = lax.rem(r + n_rows - 1, n_rows), lax.rem(r + 1, n_rows)
    left, right = lax.rem(c + n_cols - 1, n_cols), lax.rem(c + 1, n_cols)

    load_image = pltpu.make_async_copy(image_hbm, img.at[pl.ds(0, blocks), :, pl.ds(0, width)], load_sem.at[0])
    load_mask = pltpu.make_async_copy(mask_hbm, mask_v, load_sem.at[1])
    load_image.start()
    load_mask.start()

    span = 4
    depth = n_rows // span

    def peer(j):
        near = lax.rem(lax.rem(r, depth) + lax.div(j, span), depth)
        return lax.rem(lax.div(r, depth) + lax.rem(j, span), span) * depth + near

    barrier = pltpu.get_barrier_semaphore()
    odd = lax.rem(c, 2) == 1
    even = jnp.logical_not(odd)
    opposite = n_cols // 2

    def across(signal):
        for n in range(opposite):
            signal(r, lax.rem(c + 2 * n + 1, n_cols))
        for row in (up, down):
            for col in (left, right):
                signal(row, col)

    def greet(row, col):
        pl.semaphore_signal(barrier, inc=1, device_id=(row, col), device_id_type=MESH)

    def answer(row, col):
        pl.semaphore_signal(ready, inc=1, device_id=(row, col), device_id_type=MESH)

    @pl.when(even)
    def _():
        across(greet)

    for n in range(1, opposite):
        greet(r, lax.rem(c + 2 * n, n_cols))

    @pl.loop(1, n_rows)
    def _(j):
        greet(peer(j), c)

    total = n_rows * blocks
    own = jnp.broadcast_to(owner_ref[...], (total, total))
    before = lax.broadcasted_iota(jnp.int32, (total, total), 0)
    after = lax.broadcasted_iota(jnp.int32, (total, total), 1)
    same = (own == own.T) & (before < after)
    rank = jnp.sum(jnp.where(same, 1, 0), axis=0, keepdims=True)
    place = jnp.broadcast_to(owner_ref[...] * blocks + rank, (total, total)).T
    order_v[...] = jnp.sum(jnp.where(place == after, before, 0), axis=0, keepdims=True)
    to_scalars = pltpu.make_async_copy(order_v, order_s, order_sem)
    to_scalars.start()

    load_image.wait()
    load_mask.wait()

    sub = lax.broadcasted_iota(jnp.int32, (BR, TW), 0)
    lane = lax.broadcasted_iota(jnp.int32, (BR, TW), 1)
    sub_w = lax.broadcasted_iota(jnp.int32, (BR, width), 0)
    last, last_t = blocks - 1, tiles - 1

    def stage(block, m, value):
        for q in range(2):
            staged[q, m, block] = value[q * PAIR : (q + 1) * PAIR]

    def at(t):
        return pl.ds(t * TW if isinstance(t, int) else pl.multiple_of(t * TW, TW), TW)

    def coefficients(i, where):
        f = fid[i, :, where] * tau_step
        g = 1.0 / (1.0 + f)
        gain[i, :, where] = g
        bias[i, :, where] = f * img[i, :, where] * g

    @pl.loop(0, blocks)
    def _(i):
        for t in range(tiles):
            weight = weight_ref[i, t].astype(jnp.float32) * fidelity_scale
            fid[i, :, at(t)] = weight * (1 - mask_v[i, :, at(t)]).astype(jnp.float32)
            coefficients(i, at(t))
            value = img[i, :, at(t)]
            prim[i, :, at(t)] = value
            ext[i, :, at(t)] = value
            dual_r[i, :, at(t)] = jnp.zeros((BR, TW), jnp.float32)
            dual_c[i, :, at(t)] = jnp.zeros((BR, TW), jnp.float32)

    row_msg[0] = jnp.where(sub_w < HALF, img[0, :, pl.ds(0, width)], pltpu.roll(fid[0, :, pl.ds(0, width)], HALF, 0))
    row_msg[1] = jnp.where(
        sub_w >= HALF, img[last, :, pl.ds(0, width)], pltpu.roll(fid[last, :, pl.ds(0, width)], HALF, 0)
    )
    rows_here = blocks * BR
    for side, start in ((0, 0), (1, width - TW)):
        both = jnp.concatenate(
            [
                img[pl.ds(0, blocks), :, pl.ds(start, TW)].reshape(rows_here, TW),
                fid[pl.ds(0, blocks), :, pl.ds(start, TW)].reshape(rows_here, TW),
            ],
            axis=0,
        ).T
        col_msg[side] = both[:BR] if side == 0 else both[TW - BR :]

    first_tile, last_tile = pl.ds(0, TW), pl.ds(width - TW, TW)
    messages = (
        (row_msg.at[0], row_got.at[0], up, c),
        (row_msg.at[1], row_got.at[1], down, c),
        (col_msg.at[0], col_got.at[0], r, left),
        (col_msg.at[1], col_got.at[1], r, right),
        (row_msg.at[0, :, first_tile], corner_got.at[0], up, left),
        (row_msg.at[0, :, last_tile], corner_got.at[1], up, right),
        (row_msg.at[1, :, first_tile], corner_got.at[2], down, left),
        (row_msg.at[1, :, last_tile], corner_got.at[3], down, right),
    )
    halos = [
        pltpu.make_async_remote_copy(
            src_ref=src, dst_ref=dst, send_sem=halo_send.at[k], recv_sem=halo_recv.at[k],
            device_id=(row, col), device_id_type=MESH,
        )
        for k, (src, dst, row, col) in enumerate(messages)
    ]

    @pl.when(odd)
    def _():
        pl.semaphore_wait(barrier, n_rows - 1 + n_cols - 1 + 4)
        across(answer)
        for halo in halos[2:] + halos[:2]:
            halo.start()

    def dual_update(e, e_right, e_below, dr, dc, no_row=None, no_col=None):
        grad_r = pltpu.roll(jnp.where(sub == 0, e_below, e), BR - 1, 0) - e
        grad_c = pltpu.roll(jnp.where(lane == 0, e_right, e), TW - 1, 1) - e
        if no_row is not None:
            grad_r = jnp.where(sub == no_row, 0.0, grad_r)
        if no_col is not None:
            grad_c = jnp.where(lane == no_col, 0.0, grad_c)
        trial_r, trial_c = dr + sigma_step * grad_r, dc + sigma_step * grad_c
        scale = jnp.minimum(1.0, tv_weight * lax.rsqrt(trial_r * trial_r + trial_c * trial_c))
        return trial_r * scale, trial_c * scale, jnp.sqrt(grad_r * grad_r + grad_c * grad_c)

    def primal_update(p, dr, dc, dr_above, dc_left, g, b):
        upper = pltpu.roll(jnp.where(sub == BR - 1, dr_above, dr), 1, 0)
        before = pltpu.roll(jnp.where(lane == TW - 1, dc_left, dc), 1, 1)
        return (p + tau_step * ((dr - upper) + (dc - before))) * g + b

    def loss(variation, f, misfit):
        return tv_weight * variation + 0.5 * f * (misfit * misfit)

    zero = jnp.zeros((BR, TW), jnp.float32)

    @pl.loop(0, ITERS)
    def _(step):
        partial = [zero, zero]
        for i in range(blocks):
            for t in range(tiles):
                e = ext[i, :, at(t)]
                dr, dc, variation = dual_update(
                    e, ext[i, :, at(min(t + 1, last_t))], ext[min(i + 1, last), :, at(t)],
                    dual_r[i, :, at(t)], dual_c[i, :, at(t)],
                )
                dual_r[i, :, at(t)] = dr
                dual_c[i, :, at(t)] = dc
                p = prim[i, :, at(t)]
                updated = primal_update(
                    p, dr, dc, dual_r[max(i - 1, 0), :, at(t)], dual_c[i, :, at(max(t - 1, 0))],
                    gain[i, :, at(t)], bias[i, :, at(t)],
                )
                ext[i, :, at(t)] = 2.0 * updated - p
                prim[i, :, at(t)] = updated
                term = loss(variation, fid[i, :, at(t)], updated - img[i, :, at(t)])
                if i in (0, last):
                    term = jnp.where(sub >= HALF if i == 0 else sub < HALF, term, 0.0)
                if t in (0, last_t):
                    term = jnp.where(lane >= TW // 2 if t == 0 else lane < TW // 2, term, 0.0)
                partial[t % 2] = partial[t % 2] + term
        acc[step] = partial[0] + partial[1]

    for i in range(blocks):
        for t in range(1, last_t):
            value = prim[i, :, at(t)]
            stage(i, 2 * t, value[:HALF])
            stage(i, 2 * t + 1, value[HALF:])

    def spread_to(q, m, start, size):
        piece = pl.ds(start, size)
        return pltpu.make_async_remote_copy(
            src_ref=staged.at[q, m, piece], dst_ref=spread[q].at[r, piece], send_sem=send1.at[q], recv_sem=recv1.at[q],
            device_id=(m, c), device_id_type=MESH,
        )

    @pl.when(even)
    def _():
        pl.semaphore_wait(barrier, n_rows - 1 + opposite - 1)
        for halo in halos[:2]:
            halo.start()

    @pl.loop(1, n_rows)
    def _(j):
        m = peer(j)

        @pl.when((m >= 2) & (m < n_rows - 2))
        def _():
            spread_to(0, m, 1 - lax.rem(m, 2), last).start()

    for halo in halos[:2]:
        halo.wait_recv()

    below, above = row_got[0], row_got[1]
    img[blocks, :, pl.ds(0, width)] = jnp.where(sub_w < HALF, below, above)
    fid[blocks, :, pl.ds(0, width)] = pltpu.roll(jnp.where(sub_w < HALF, above, below), HALF, 0)
    coefficients(blocks, pl.ds(0, width))

    rows_of, cols_of = (last, blocks, 0), (last_t, tiles, 0)
    no_rows = (jnp.where(r == n_rows - 1, BR - 1, BR), jnp.where(r == 0, BR - 1, BR), None)
    no_cols = (jnp.where(c == n_cols - 1, TW - 1, TW), jnp.where(c == 0, TW - 1, TW), None)

    for k in range(3):
        for t in range(tiles):
            value = img[rows_of[k], :, at(t)]
            strip_prim[k, :, at(t)] = value
            strip_ext[k, :, at(t)] = value
            strip_r[k, :, at(t)] = zero
            strip_c[k, :, at(t)] = zero

    @pl.loop(0, ITERS)
    def _(step):
        partial = acc[step]
        for t in range(tiles):
            e = [strip_ext[k, :, at(t)] for k in range(3)]
            duals = []
            for k in range(3):
                duals.append(
                    dual_update(
                        e[k], strip_ext[k, :, at(min(t + 1, last_t))], e[(k + 1) % 3],
                        strip_r[k, :, at(t)], strip_c[k, :, at(t)], no_row=no_rows[k],
                    )
                )
            for k in range(3):
                dr, dc, variation = duals[k]
                strip_r[k, :, at(t)] = dr
                strip_c[k, :, at(t)] = dc
                p = strip_prim[k, :, at(t)]
                i = rows_of[k]
                updated = primal_update(
                    p, dr, dc, duals[(k + 2) % 3][0], strip_c[k, :, at(max(t - 1, 0))],
                    gain[i, :, at(t)], bias[i, :, at(t)],
                )
                strip_ext[k, :, at(t)] = 2.0 * updated - p
                strip_prim[k, :, at(t)] = updated
                if k != 1:
                    term = loss(variation, fid[i, :, at(t)], updated - img[i, :, at(t)])
                    term = jnp.where(sub < HALF if k == 2 else sub >= HALF, term, 0.0)
                    if t in (0, last_t):
                        term = jnp.where(lane >= TW // 2 if t == 0 else lane < TW // 2, term, 0.0)
                    partial = partial + term
        acc[step] = partial

    for t in range(1, last_t):
        stage(0, 2 * t, strip_prim[2, :HALF, at(t)])
        stage(last, 2 * t + 1, strip_prim[0, HALF:, at(t)])

    @pl.loop(1, n_rows)
    def _(j):
        m = peer(j)

        @pl.when((m >= 2) & (m < n_rows - 2))
        def _():
            spread_to(0, m, last * lax.rem(m, 2), 1).start()

    @pl.when(even)
    def _():
        pl.semaphore_wait(ready, opposite + 4)
        for halo in halos[2:]:
            halo.start()

    @pl.loop(1, n_rows)
    def _(j):
        m = peer(j)

        @pl.when((m >= 2) & (m < n_rows - 2))
        def _():
            spread_to(1, m, 0, blocks).start()

    n_edges = 2 * BR
    inner = (r >= 2) & (r < n_rows - 2)
    holds_edge = lax.rem(r, 2) == 0
    no_edge = jnp.logical_not(holds_edge)
    mine = lax.div(r, 2)

    to_scalars.wait()

    def batch(src, dst, count, send_sem, recv_sem):
        some = pl.ds(0, count)
        return pltpu.make_async_remote_copy(
            src_ref=src.at[some], dst_ref=dst.at[some], send_sem=send_sem, recv_sem=recv_sem,
            device_id=(up, c), device_id_type=MESH,
        )

    group = 4

    def targets_of(q):
        return [peer(q * group + n) for n in range(group)]

    def sort_for(source, target, targets):
        values = []
        for d in targets:
            for k in range(blocks):
                values.append(source(order_s[0, d * blocks + k]))
        for n, value in enumerate(values):
            target(targets[n // blocks], n % blocks, value)

    def sort_and_send(source, target, collect):
        sort_for(source, target, targets_of(0))

        @pl.loop(1, n_rows // group)
        def _(q):
            sort_for(source, target, targets_of(q))
            for n in range(group):
                before = (q - 1) * group + n

                @pl.when(before > 0)
                def _():
                    collect(peer(before)).start()

        for n in range(group):
            collect(peer(n_rows - group + n)).start()

    def second_stage(q):
        def collect_to(d):
            return pltpu.make_async_remote_copy(
                src_ref=sorted_.at[q, d], dst_ref=gathered.at[q, r], send_sem=send2.at[q], recv_sem=recv2.at[q],
                device_id=(d, c), device_id_type=MESH,
            )

        def source(b):
            return spread[q][lax.div(b, blocks), lax.rem(b, blocks)]

        def target(d, k, value):
            sorted_[q, d, k] = value

        @pl.when(inner)
        def _():
            spread[q][r] = staged[q, r]
            batch(staged.at[q], spread[q], n_rows - 1, send1.at[q], recv1.at[q]).wait_recv()
            sort_and_send(source, target, collect_to)
            gathered[q, r] = sorted_[q, r]

    for halo in halos[2:]:
        halo.wait_recv()

    sides = jnp.concatenate([col_got[0], jnp.zeros((TW - 2 * BR, TW), jnp.float32), col_got[1]], axis=0).T
    img[pl.ds(0, blocks), :, pl.ds(width, TW)] = sides[:rows_here].reshape(blocks, BR, TW)
    fid[pl.ds(0, blocks), :, pl.ds(width, TW)] = sides[rows_here:].reshape(blocks, BR, TW)
    low = jnp.where(lane < TW // 2, corner_got[0], corner_got[1])
    high = jnp.where(lane < TW // 2, corner_got[2], corner_got[3])
    img[blocks, :, pl.ds(width, TW)] = jnp.where(sub < HALF, low, high)
    fid[blocks, :, pl.ds(width, TW)] = pltpu.roll(jnp.where(sub < HALF, high, low), HALF, 0)
    for i in range(blocks + 1):
        coefficients(i, at(tiles))
    for i in range(blocks + 1):
        for k in range(3):
            value = img[i, :, at(cols_of[k])]
            side_prim[i, :, at(k)] = value
            side_ext[i, :, at(k)] = value
            side_r[i, :, at(k)] = zero
            side_c[i, :, at(k)] = zero

    @pl.loop(0, ITERS)
    def _(step):
        partial = acc[step]
        variations = {}
        e = [[side_ext[i, :, at(k)] for k in range(3)] for i in range(blocks + 1)]
        for i in range(blocks + 1):
            no_row = no_rows[0] if i == last else no_rows[1] if i == blocks else None
            for k in range(3):
                dr, dc, variations[i, k] = dual_update(
                    e[i][k], e[i][(k + 1) % 3], e[(i + 1) % (blocks + 1)][k],
                    side_r[i, :, at(k)], side_c[i, :, at(k)], no_row=no_row, no_col=no_cols[k],
                )
                side_r[i, :, at(k)] = dr
                side_c[i, :, at(k)] = dc
        for i in range(blocks + 1):
            for k in range(3):
                t = cols_of[k]
                p = side_prim[i, :, at(k)]
                updated = primal_update(
                    p, side_r[i, :, at(k)], side_c[i, :, at(k)], side_r[(i + blocks) % (blocks + 1), :, at(k)],
                    side_c[i, :, at((k + 2) % 3)], gain[i, :, at(t)], bias[i, :, at(t)],
                )
                side_ext[i, :, at(k)] = 2.0 * updated - p
                side_prim[i, :, at(k)] = updated
                if k != 1 and i < blocks:
                    term = loss(variations[i, k], fid[i, :, at(t)], updated - img[i, :, at(t)])
                    partial = partial + jnp.where(lane < TW // 2 if k == 2 else lane >= TW // 2, term, 0.0)
        acc[step] = partial

    for side, k, t in ((0, 2, 0), (1, 0, last_t)):
        for i in range(blocks):
            value = prim[i, :, at(t)]
            if i == 0:
                value = jnp.where(sub < HALF, strip_prim[2, :, at(t)], value)
            if i == last:
                value = jnp.where(sub >= HALF, strip_prim[0, :, at(t)], value)
            value = jnp.where(lane < TW // 2 if k == 2 else lane >= TW // 2, side_prim[i, :, at(k)], value)
            for q in range(BR):
                edge_staged[side * BR + q, i] = value[q : q + 1]

    lane_1 = lax.broadcasted_iota(jnp.int32, (1, TW), 1)
    sums = jnp.zeros((1, TW), jnp.float32)
    for step in range(ITERS):
        line = jnp.sum(acc[step], axis=0, keepdims=True)
        sums = jnp.where(lane_1 == step, jnp.sum(line, axis=1, keepdims=True), sums)
    part_src_c[...] = sums
    part_cols[c] = sums

    def part_across(col):
        return pltpu.make_async_remote_copy(
            src_ref=part_src_c, dst_ref=part_cols.at[c], send_sem=csend, recv_sem=crecv,
            device_id=(r, col), device_id_type=MESH,
        )

    @pl.loop(1, n_cols)
    def _(j):
        part_across(lax.rem(c + j, n_cols)).start()

    def edge_to(u):
        return pltpu.make_async_remote_copy(
            src_ref=edge_staged.at[u], dst_ref=edge_spread.at[pl.ds(r * blocks, blocks)],
            send_sem=esend1, recv_sem=erecv1, device_id=(2 * u, c), device_id_type=MESH,
        )

    @pl.loop(0, n_edges)
    def _(j):
        u = lax.rem(mine + j, n_edges)

        @pl.when(2 * u != r)
        def _():
            edge_to(u).start()

    @pl.when(holds_edge)
    def _():
        for i in range(blocks):
            edge_spread[r * blocks + i] = edge_staged[mine, i]

    second_stage(0)
    second_stage(1)

    def edge_collect_to(d):
        return pltpu.make_async_remote_copy(
            src_ref=edge_sorted.at[d], dst_ref=edge_gathered.at[mine], send_sem=esend2, recv_sem=erecv2,
            device_id=(d, c), device_id_type=MESH,
        )

    @pl.when(holds_edge)
    def _():
        arrived = pl.ds(0, (n_rows - 1) * blocks)
        pltpu.make_async_remote_copy(
            src_ref=edge_spread.at[arrived], dst_ref=edge_spread.at[arrived], send_sem=esend1, recv_sem=erecv1,
            device_id=(up, c), device_id_type=MESH,
        ).wait_recv()

        def target(d, k, value):
            edge_sorted[d, k] = value

        sort_and_send(lambda b: edge_spread[b], target, edge_collect_to)
        edge_gathered[mine] = edge_sorted[r]

    col_peers = pl.ds(0, n_cols - 1)
    all_cols = pltpu.make_async_remote_copy(
        src_ref=part_cols.at[col_peers], dst_ref=part_cols.at[col_peers], send_sem=csend, recv_sem=crecv,
        device_id=(r, left), device_id_type=MESH,
    )
    all_cols.wait_recv()
    here = part_cols[0]
    for n in range(1, n_cols):
        here = here + part_cols[n]
    part_src[...] = here
    part_rows[r] = here

    def part_to(m):
        return pltpu.make_async_remote_copy(
            src_ref=part_src, dst_ref=part_rows.at[r], send_sem=psend, recv_sem=precv,
            device_id=(m, c), device_id_type=MESH,
        )

    @pl.loop(1, n_rows)
    def _(j):
        part_to(peer(j)).start()

    all_parts = batch(part_rows, part_rows, n_rows - 1, psend, precv)
    all_parts.wait_recv()
    everywhere = part_rows[0]
    for n in range(1, n_rows):
        everywhere = everywhere + part_rows[n]
    objective_ref[...] = everywhere / pixel_total

    for halo in halos:
        halo.wait_send()
    all_parts.wait_send()
    all_cols.wait_send()
    pieces = n_rows - 4

    for q in range(2):
        first = functools.partial(batch, staged.at[q], spread[q], send_sem=send1.at[q], recv_sem=recv1.at[q])
        second = functools.partial(batch, sorted_.at[q], gathered.at[q], send_sem=send2.at[q], recv_sem=recv2.at[q])

        @pl.when(inner)
        def _():
            first(pieces - 1).wait_send()
            second(n_rows - 1).wait_send()
            second(pieces - 1).wait_recv()

        @pl.when(jnp.logical_not(inner))
        def _():
            first(pieces).wait_send()
            second(pieces).wait_recv()

    @pl.when(holds_edge)
    def _():
        batch(edge_staged, edge_gathered, n_edges - 1, esend1, erecv1).wait_send()
        batch(edge_sorted, edge_sorted, n_rows - 1, esend2, erecv2).wait_send()
        batch(edge_gathered, edge_gathered, n_edges - 1, esend2, erecv2).wait_recv()

    @pl.when(no_edge)
    def _():
        batch(edge_staged, edge_gathered, n_edges, esend1, erecv1).wait_send()
        batch(edge_gathered, edge_gathered, n_edges, esend2, erecv2).wait_recv()


def assemble(pieces, edges, row, out_hbm, objective, out, sems):
    blocks, _, width = out.shape
    stores = [pltpu.make_async_copy(out.at[k], out_hbm.at[k], sems.at[k]) for k in range(blocks)]
    for k in range(blocks):
        for t in range(1, width // TW - 1):
            out[k, :, pl.ds(t * TW, TW)] = jnp.concatenate([pieces[q, 2 * t + h, k] for h in range(2) for q in range(2)], axis=0)
        for side, start in ((0, 0), (1, width - TW)):
            out[k, :, pl.ds(start, TW)] = jnp.concatenate([edges[side * BR + q, k] for q in range(BR)], axis=0)
        stores[k].start()
    lanes = lax.broadcasted_iota(jnp.int32, (1, TW), 1)
    for step in range(ITERS):
        objective[step] = jnp.sum(jnp.where(lanes == step, row[...], 0.0))
    for store in stores:
        store.wait()


def per_device(n_rows, n_cols, image, cloud_mask, tile_weight, owner):
    rows_here, width = image.shape
    blocks = rows_here // BR
    tiles = width // TW
    pixel_total = float(n_rows * n_cols * rows_here * width)
    f32 = jnp.float32
    ringed = pltpu.VMEM((blocks + 1, BR, width + TW), f32)
    half = pltpu.VMEM((n_rows, blocks, PAIR, TW), f32)
    pieces = pltpu.VMEM((2, n_rows, blocks, PAIR, TW), f32)
    dma = pltpu.SemaphoreType.DMA
    scratch = (
        [ringed] * 4
        + [pltpu.VMEM((blocks, BR, width), f32)] * 4
        + [pltpu.VMEM((3, BR, width), f32)] * 4
        + [pltpu.VMEM((blocks + 1, BR, 3 * TW), f32)] * 4
        + [
            pltpu.VMEM((blocks, BR, width), jnp.int32),
            pltpu.VMEM((2, BR, width), f32),
            pltpu.VMEM((2, BR, width), f32),
            pltpu.VMEM((2, BR, TW), f32),
            pltpu.VMEM((2, BR, TW), f32),
            pltpu.VMEM((4, BR, TW), f32),
        ]
        + [pieces, half, half, pieces]
        + [pltpu.VMEM((n, 1, TW) if n > 99 else (n, blocks, 1, TW), f32) for n in (2 * BR, n_rows * blocks, n_rows)]
        + [
            pltpu.VMEM((1, n_rows * blocks), jnp.int32),
            pltpu.SMEM((1, n_rows * blocks), jnp.int32),
            pltpu.VMEM((ITERS, BR, TW), f32),
            pltpu.VMEM((1, TW), f32),
            pltpu.VMEM((n_rows, 1, TW), f32),
            pltpu.VMEM((1, TW), f32),
            pltpu.VMEM((n_cols, 1, TW), f32),
            dma((2,)), dma, dma((8,)), dma((8,)),
            dma((2,)), dma((2,)), dma((2,)), dma((2,)), dma, dma, dma, dma, dma, dma, dma, dma,
            pltpu.SemaphoreType.REGULAR,
        ]
    )
    vmem, smem, hbm = (pl.BlockSpec(memory_space=s) for s in (pltpu.VMEM, pltpu.SMEM, pl.ANY))
    received, edges, row = pl.pallas_call(
        functools.partial(kernel, n_rows, n_cols, blocks, tiles, pixel_total),
        out_shape=(
            pieces,
            pltpu.VMEM((2 * BR, blocks, 1, TW), f32),
            pltpu.VMEM((1, TW), f32),
        ),
        in_specs=[hbm, hbm, smem, vmem],
        out_specs=(vmem, vmem, vmem),
        scratch_shapes=scratch,
        compiler_params=pltpu.CompilerParams(collective_id=0, has_side_effects=True),
    )(
        image.reshape(blocks, BR, width),
        cloud_mask.reshape(blocks, BR, width),
        tile_weight,
        owner.reshape(1, -1),
    )
    out, objective = pl.pallas_call(
        assemble,
        out_shape=(jax.ShapeDtypeStruct((blocks, BR, width), f32), jax.ShapeDtypeStruct((ITERS,), f32)),
        in_specs=[vmem, vmem, vmem],
        out_specs=(hbm, smem),
        scratch_shapes=[pltpu.VMEM((blocks, BR, width), f32), dma((blocks,))],
    )(*(pltpu.with_memory_space_constraint(x, pltpu.VMEM) for x in (received, edges, row)))
    return out.reshape(rows_here, width), objective


def solution(mesh):
    placed = (P("rows", "cols"), P("rows", "cols"), P("rows", "cols"), P())
    return jax.shard_map(
        functools.partial(per_device, mesh.shape["rows"], mesh.shape["cols"]),
        mesh=mesh, in_specs=placed, out_specs=(P("rows", "cols"), P()), check_vma=False,
    )
```
